256 devices in a mesh: row: 32 (over y, x, core), col: 8 (over z).
Axes of the slice: x: 4, y: 4, z: 8, core: 2. Of those that a mesh axis runs over, the one named last changes fastest.
Arguments:
- sources: float32 [3, 4096, 8192], P(None, 'row', 'col'), may hold values from -32 to 32
- labels: int32 [4096, 8192], P('row', 'col'), may hold values from 0 to 2
Outputs:
- blended: float32 [4096, 8192], P('row', 'col')
- overview_fine: float32 [2048, 4096], P('row', 'col')
- overview_mid: float32 [1024, 2048], P(None, 'col')
- overview_coarse: float32 [512, 1024], P(None, 'col')
The draws below stay inside these ranges and needn't reach their ends.
All inputs are finite; a program needn't handle non-finite values.
Results may differ from the reference program's by a relative error of at most 0.0001.
Values sent between devices are 32-bit elements; how exact they have to be, the bound alone decides.
A program may use at most 64 MiB of HBM per device.

```python
import jax
import jax.numpy as jnp

K = 3
ITERS = 3
H = 4096
W = 8192


def draw_sources(key, part):
    row_frac = jnp.arange(H, dtype=jnp.float32) / H
    col_frac = jnp.arange(W, dtype=jnp.float32) / W
    amplitude = (1.0 + 2.0 * row_frac)[:, None] * (1.0 + 2.0 * col_frac)[None, :] / 3.0
    noise_draw = jnp.clip(jax.random.normal(key, (K, H, W), jnp.float32), -6.0, 6.0)
    return noise_draw * amplitude


def touch_ends(entries, own_key, smallest, top_value):
    place = [jax.random.randint(jax.random.fold_in(own_key, axis), (), 0, length) for axis, length in enumerate(entries.shape)]
    main_axis = entries.shape.index(max(entries.shape))
    neighbour = place[:main_axis] + [(place[main_axis] + 1) % entries.shape[main_axis]] + place[main_axis + 1:]
    return entries.at[tuple(place)].set(smallest).at[tuple(neighbour)].set(top_value)


def setup_inputs(seed: int = 0) -> dict:
    key_of = jax.random.split(jax.random.key(seed), 3)
    return {
        "sources": draw_sources(jax.random.fold_in(key_of[2], 71), 0),
        "labels": touch_ends(jax.random.randint(key_of[1], (H, W), 0, K), jax.random.fold_in(key_of[1], 1), 0, K - 1).astype(jnp.int32),
    }


def apply_stencil(values):
    padded = jnp.pad(values, 1)
    beside = padded[2:, 1:-1] + padded[:-2, 1:-1]
    beside = beside + padded[1:-1, 2:] + padded[1:-1, :-2]
    return 4.0 * values - beside


def average_pool(values):
    return 0.25 * (values[0::2, 0::2] + values[1::2, 0::2] + values[0::2, 1::2] + values[1::2, 1::2])


def reference(sources, labels):
    right_side = jnp.zeros(labels.shape, jnp.float32)
    for channel in range(K):
        right_side = right_side + jnp.where(labels == channel, apply_stencil(sources[channel]), jnp.float32(0.0))
    blended = jnp.zeros(labels.shape, jnp.float32)
    residual = right_side
    direction = right_side
    norm_now = jnp.sum(residual * residual)
    for iteration in range(ITERS):
        applied = apply_stencil(direction)
        step_size = norm_now / jnp.sum(direction * applied)
        blended = blended + step_size * direction
        residual = residual - step_size * applied
        norm_next = jnp.sum(residual * residual)
        direction = residual + (norm_next / norm_now) * direction
        norm_now = norm_next
    overview_fine = average_pool(blended)
    overview_mid = average_pool(overview_fine)
    overview_coarse = average_pool(overview_mid)
    return (blended, overview_fine, overview_mid, overview_coarse)
```

```python
import jax
import jax.numpy as jnp
from jax import lax
from jax.experimental import pallas as pl
from jax.experimental.pallas import tpu as pltpu
from jax.sharding import PartitionSpec as P

MESH = pl.DeviceIdType.MESH
F32 = jnp.float32
T = 8
ROWS = 144
LANE_ROLL = 127


def two_sum(a, b):
    s = a + b
    t = s - a
    return s, (a - (s - t)) + (b - t)


def dd_add(a, b):
    s, e = two_sum(a[0], b[0])
    return two_sum(s, e + (a[1] + b[1]))


def dd_neg(a):
    return (-a[0], -a[1])


def dd_sub(a, b):
    return dd_add(a, dd_neg(b))


def split(a):
    t = a * 4097.0
    hi = t - (t - a)
    return hi, a - hi


def two_prod(a, b):
    p = a * b
    ah, al = split(a)
    bh, bl = split(b)
    return p, ((ah * bh - p) + ah * bl + al * bh) + al * bl


def dd_mul(a, b):
    p, e = two_prod(a[0], b[0])
    return two_sum(p, e + (a[0] * b[1] + a[1] * b[0]))


def dd_div(a, b):
    q = a[0] / b[0]
    p, e = two_prod(q, b[0])
    r = ((a[0] - p) - e) + (a[1] - q * b[1])
    return two_sum(q, r / b[0])


def krylov_weights(n):
    l1 = dd_div(n[2], n[1])
    l2 = dd_div(n[3], n[1])
    d1 = dd_sub(n[3], dd_mul(l1, n[2]))
    e = dd_sub(n[4], dd_mul(l1, n[3]))
    l3 = dd_div(e, d1)
    d2 = dd_sub(dd_sub(n[5], dd_mul(l2, n[3])), dd_mul(l3, e))
    y1 = dd_sub(n[1], dd_mul(l1, n[0]))
    y2 = dd_sub(dd_sub(n[2], dd_mul(l2, n[0])), dd_mul(l3, y1))
    ok1 = d1[0] > 1e-10 * n[3][0]
    ok2 = ok1 & (d2[0] > 1e-10 * n[5][0])
    c2 = tuple(jnp.where(ok2, v, 0.0) for v in dd_div(y2, d2))
    c1 = dd_sub(dd_div(y1, d1), dd_mul(l3, c2))
    c1 = tuple(jnp.where(ok1, v, 0.0) for v in c1)
    c0 = dd_sub(dd_sub(dd_div(n[0], n[1]), dd_mul(l1, c1)), dd_mul(l2, c2))
    return c0[0], c1[0], c2[0]


def pool_lanes(pair):
    src = lax.broadcasted_iota(jnp.int32, (256, 128), 0)
    dst = lax.broadcasted_iota(jnp.int32, (256, 128), 1)
    weight = jnp.where(src // 2 == dst, 0.25, 0.0).astype(jnp.bfloat16)
    hi = pair.astype(jnp.bfloat16)
    rest = pair - hi.astype(F32)
    mid = rest.astype(jnp.bfloat16)
    low = (rest - mid.astype(F32)).astype(jnp.bfloat16)
    dot = lambda v: jnp.dot(v, weight, preferred_element_type=F32)
    return dot(hi) + dot(mid) + dot(low)


def make_kernel(n_row, n_col):
    n_chip = n_row // 2

    def kernel(src, lab, o_blend, o_fine, o_mid, o_coarse,
               E, L, V, O, FI, GM, CO, strip, strip_in, corner_in, corner_lab,
               msg, red_row, red_col,
               load_sem, halo_send, halo_recv, red_send, red_recv,
               g_send, g_recv, out_sem):
        row = lax.axis_index("row")
        col = lax.axis_index("col")
        has_up, has_down = row > 0, row < n_row - 1
        has_left, has_right = col > 0, col < n_col - 1

        loads = []
        for j in range(T):
            lanes = pl.ds(128 * j, 128)
            loads.append(pltpu.make_async_copy(
                src.at[:, :, lanes], E.at[:, j, pl.ds(8, 128), :], load_sem.at[2 * j]))
            loads.append(pltpu.make_async_copy(
                lab.at[:, lanes], L.at[j, pl.ds(8, 128), :], load_sem.at[2 * j + 1]))
        for cp in loads:
            cp.start()

        barrier = pltpu.get_barrier_semaphore()

        @pl.loop(1, n_row)
        def _(i):
            pl.semaphore_signal(barrier, inc=1, device_id={"row": (row + i) % n_row, "col": col},
                                device_id_type=MESH)

        @pl.loop(1, n_col)
        def _(i):
            pl.semaphore_signal(barrier, inc=1, device_id={"row": row, "col": (col + i) % n_col},
                                device_id_type=MESH)

        diagonal = ((-1, -1, has_up & has_left), (-1, 1, has_up & has_right),
                    (1, -1, has_down & has_left), (1, 1, has_down & has_right))
        expected = n_row + n_col - 2
        for dr, dc, there in diagonal:
            @pl.when(there)
            def _(dr=dr, dc=dc):
                pl.semaphore_signal(barrier, inc=1, device_id={"row": row + dr, "col": col + dc},
                                    device_id_type=MESH)
            expected = expected + there.astype(jnp.int32)

        @pl.when(jnp.logical_not(has_up))
        def _():
            E[:, 0:T, 0:8, :] = jnp.zeros((3, T, 8, 128), F32)
            L[0:T, 0:8, :] = jnp.zeros((T, 8, 128), jnp.int32)

        @pl.when(jnp.logical_not(has_down))
        def _():
            E[:, 0:T, 136:144, :] = jnp.zeros((3, T, 8, 128), F32)
            L[0:T, 136:144, :] = jnp.zeros((T, 8, 128), jnp.int32)

        for cp in loads:
            cp.wait()

        lane = lax.broadcasted_iota(jnp.int32, (128, 128), 1)
        packed = jnp.zeros((128, 128), F32)
        for k in range(4):
            if k < 3:
                first, last = E[k, 0, 8:136, :], E[k, T - 1, 8:136, :]
            else:
                first, last = L[0, 8:136, :].astype(F32), L[T - 1, 8:136, :].astype(F32)
            both = pltpu.roll(jnp.where(lane < 64, first, last), 8 * k + 4, axis=1)
            packed = jnp.where((lane >= 8 * k) & (lane < 8 * k + 8), both, packed)
        strip[...] = packed.T[0:32, :]

        pl.semaphore_wait(barrier, expected)

        def to(r, c):
            return dict(device_id={"row": r, "col": c}, device_id_type=MESH)

        halo = []

        def exchange(slot, s_ref, d_ref, goes, r, c, comes):
            cp = pltpu.make_async_remote_copy(
                src_ref=s_ref, dst_ref=d_ref, send_sem=halo_send.at[slot],
                recv_sem=halo_recv.at[slot], **to(r, c))

            @pl.when(goes)
            def _():
                cp.start()
            halo.append((cp, goes, comes))

        exchange(0, strip, strip_in.at[0], has_right, row, col + 1, has_left)
        exchange(1, strip, strip_in.at[1], has_left, row, col - 1, has_right)
        exchange(2, E.at[:, pl.ds(0, T), pl.ds(8, 8), :], E.at[:, pl.ds(0, T), pl.ds(136, 8), :],
                 has_up, row - 1, col, has_down)
        exchange(3, E.at[:, pl.ds(0, T), pl.ds(128, 8), :], E.at[:, pl.ds(0, T), pl.ds(0, 8), :],
                 has_down, row + 1, col, has_up)
        exchange(4, L.at[pl.ds(0, T), pl.ds(8, 8), :], L.at[pl.ds(0, T), pl.ds(136, 8), :],
                 has_up, row - 1, col, has_down)
        exchange(5, L.at[pl.ds(0, T), pl.ds(128, 8), :], L.at[pl.ds(0, T), pl.ds(0, 8), :],
                 has_down, row + 1, col, has_up)
        slot = 6
        opposite = (diagonal[3][2], diagonal[2][2], diagonal[1][2], diagonal[0][2])
        for q, (dr, dc, there) in enumerate(diagonal):
            rows = pl.ds(8 if dr < 0 else 128, 8)
            j = 0 if dc < 0 else T - 1
            exchange(slot, E.at[:, j, rows, :], corner_in.at[q], there, row + dr, col + dc,
                     opposite[q])
            exchange(slot + 1, L.at[j, rows, :], corner_lab.at[q], there, row + dr, col + dc,
                     opposite[q])
            slot += 2

        for cp, goes, comes in halo:
            @pl.when(comes)
            def _(cp=cp):
                cp.wait_recv()

        sub32 = lax.broadcasted_iota(jnp.int32, (32, 128), 0) % 8
        merged = jnp.where((sub32 < 4) & has_left, strip_in[0],
                           jnp.where((sub32 >= 4) & has_right, strip_in[1], 0.0))
        beside = jnp.concatenate([merged, jnp.zeros((96, 128), F32)], axis=0).T
        outer = (lane < 4) | (lane >= 124)
        for k in range(4):
            tile = jnp.where(outer, pltpu.roll(beside, 128 - (8 * k + 4), axis=1), 0.0)
            if k < 3:
                E[k, T, 8:136, :] = tile
            else:
                L[T, 8:136, :] = tile.astype(jnp.int32)

        lane8 = lax.broadcasted_iota(jnp.int32, (8, 128), 1)
        sub8 = lax.broadcasted_iota(jnp.int32, (8, 128), 0)
        low4, high4 = lane8 < 4, lane8 >= 124
        for rows, from_left, from_right in ((slice(0, 8), 3, 2), (slice(136, 144), 1, 0)):
            l_ok, r_ok = opposite[from_left], opposite[from_right]
            for k in range(3):
                E[k, T, rows, :] = jnp.where(
                    high4 & l_ok, corner_in[from_left, k],
                    jnp.where(low4 & r_ok, corner_in[from_right, k], 0.0))
            L[T, rows, :] = jnp.where(
                high4 & l_ok, corner_lab[from_left],
                jnp.where(low4 & r_ok, corner_lab[from_right], 0))

        col_ok = (low4 & has_right) | (high4 & has_left)
        first_lane, last_lane = lane8 == 0, lane8 == 127

        def stencil(read, rows, rows_up, rows_down, count):
            c = [read(j, rows) for j in range(T + 1)]
            fwd = [pltpu.roll(v, 1, axis=1) for v in c]
            bwd = [pltpu.roll(v, 127, axis=1) for v in c]
            out = []
            for j in range(count):
                left = jnp.where(first_lane, fwd[j - 1], fwd[j])
                right = jnp.where(last_lane, bwd[(j + 1) % (T + 1)], bwd[j])
                near = (read(j, rows_down) + read(j, rows_up)) + (right + left)
                out.append(4.0 * c[j] - near)
            return c, out

        def row_slices(base):
            return pl.ds(base, 8), pl.ds(base - 1, 8), pl.ds(base + 1, 8)

        def store_field(f, rows, tiles, ok):
            for j, v in enumerate(tiles):
                if j == T:
                    v = jnp.where(col_ok, v, 0.0)
                if ok is not None:
                    v = jnp.where(ok, v, 0.0)
                V[f, j, rows, :] = v

        def right_side(base, ok):
            rows, up, down = row_slices(base)
            labels = [L[j, rows, :] for j in range(T + 1)]
            b = [None] * (T + 1)
            for k in range(3):
                _, a = stencil(lambda j, r, k=k: E[k, j, r, :], rows, up, down, T + 1)
                b = a if k == 0 else [
                    jnp.where(lb == k, v, w) for lb, v, w in zip(labels, a, b)]
            store_field(0, rows, b, ok)

        def apply(f, base, ok, count=T + 1):
            rows, up, down = row_slices(base)
            c, a = stencil(lambda j, r: V[f, j, r, :], rows, up, down, count)
            if f < 2:
                store_field(f + 1, rows, a, ok)
            return c, a

        top_ok = has_up | (sub8 == 7)
        bottom_ok = has_down | (sub8 == 0)
        right_side(1, top_ok)
        right_side(135, bottom_ok)

        @pl.loop(1, 17)
        def _(i):
            right_side(pl.multiple_of(8 * i, 8), None)

        def add_up(products):
            while len(products) > 1:
                products = [a + b for a, b in zip(products[::2], products[1::2])]
            return products[0]

        zero8 = jnp.zeros((8, 128), F32)
        sums = []
        for f in range(3):
            if f < 2:
                apply(f, 1, top_ok)
                apply(f, 135, bottom_ok)

            def body(i, carry, f=f):
                c, a = apply(f, pl.multiple_of(8 * i, 8), None, T + 1 if f < 2 else T)
                same = add_up([c[j] * c[j] for j in range(T)])
                next_ = add_up([c[j] * a[j] for j in range(T)])
                return carry[0] + same, carry[1] + next_
            sums += list(lax.fori_loop(1, 17, body, (zero8, zero8)))

        pairs = [(s, zero8) for s in sums]
        for shift in (4, 2, 1):
            pairs = [dd_add(p, (pltpu.roll(p[0], shift, axis=0), pltpu.roll(p[1], shift, axis=0)))
                     for p in pairs]
        hi, lo = zero8, zero8
        for m, p in enumerate(pairs):
            hi, lo = jnp.where(sub8 == m, p[0], hi), jnp.where(sub8 == m, p[1], lo)
        for shift in (64, 32, 16, 8, 4, 2, 1):
            hi, lo = dd_add((hi, lo), (pltpu.roll(hi, shift, axis=1), pltpu.roll(lo, shift, axis=1)))
        line = jnp.where(lane8 == sub8, hi, 0.0) + jnp.where(lane8 == sub8 + 8, lo, 0.0)
        line = jnp.sum(line, axis=0, keepdims=True)

        lane1 = lax.broadcasted_iota(jnp.int32, (1, 128), 1)

        def total(lines):
            err = []
            while len(lines) > 1:
                both = [two_sum(a, b) for a, b in zip(lines[::2], lines[1::2])]
                lines = [b[0] for b in both]
                err += [b[1] for b in both]
            err = add_up(err + [jnp.zeros((1, 128), F32)])
            low = pltpu.roll(lines[0], 120, axis=1) + err
            h, l = two_sum(lines[0], low)
            return jnp.where(lane1 < 8, h, 0.0) + jnp.where(
                (lane1 >= 8) & (lane1 < 16), pltpu.roll(l, 8, axis=1), 0.0)

        def all_reduce(line, buf, phase, n, me, device):
            msg[phase] = line
            buf[me] = line

            @pl.loop(1, n)
            def _(i):
                peer = (me + i) % n
                pltpu.make_async_remote_copy(
                    src_ref=msg.at[phase], dst_ref=buf.at[me], send_sem=red_send.at[phase],
                    recv_sem=red_recv.at[phase], device_id=device(peer),
                    device_id_type=MESH).start()
            rest = buf.at[pl.ds(0, n - 1)]
            pltpu.make_async_copy(rest, rest, red_recv.at[phase]).wait()
            pltpu.make_async_copy(rest, rest, red_send.at[phase]).wait()
            return total([buf[i] for i in range(n)])

        line = all_reduce(line, red_col, 0, n_col, col, lambda p: {"row": row, "col": p})
        line = all_reduce(line, red_row, 1, n_row, row, lambda p: {"row": p, "col": col})

        pick = lambda m: jnp.sum(jnp.where(lane1 == m, line, 0.0), axis=1, keepdims=True)
        n = [(pick(m), pick(m + 8)) for m in range(6)]
        c0, c1, c2 = (jnp.broadcast_to(c, (8, 128)) for c in krylov_weights(n))

        @pl.loop(0, 16)
        def _(i):
            r = pl.multiple_of(8 * i, 8)
            for j in range(T):
                O[j, pl.ds(r, 8), :] = (
                    c0 * V[0, j, pl.ds(r + 8, 8), :] + c1 * V[1, j, pl.ds(r + 8, 8), :]
                    + c2 * V[2, j, pl.ds(r + 8, 8), :])

        outs = [pltpu.make_async_copy(O.at[j], o_blend.at[:, pl.ds(128 * j, 128)], out_sem.at[j])
                for j in range(T)]
        for cp in outs:
            cp.start()

        for j in range(T // 2):
            rows = [O[2 * j + h, pl.ds(0, 64, stride=2), :] + O[2 * j + h, pl.ds(1, 64, stride=2), :]
                    for h in range(2)]
            FI[j] = pool_lanes(jnp.concatenate(rows, axis=1))
        for j in range(T // 4):
            rows = [FI[2 * j + h, pl.ds(0, 32, stride=2), :] + FI[2 * j + h, pl.ds(1, 32, stride=2), :]
                    for h in range(2)]
            GM[row, j] = pool_lanes(jnp.concatenate(rows, axis=1))

        chip, core = row // 2, row % 2
        partner = 2 * chip + 1 - core

        def block_copy(r, target, sem):
            return pltpu.make_async_remote_copy(
                src_ref=GM.at[r], dst_ref=GM.at[r], send_sem=g_send.at[sem], recv_sem=g_recv.at[r],
                **to(target, col))

        @pl.loop(1, n_chip)
        def _(i):
            block_copy(row, 2 * ((chip + i) % n_chip) + core, i).start()
        block_copy(row, partner, 0).start()

        for j in range(T // 2):
            cp = pltpu.make_async_copy(FI.at[j], o_fine.at[:, pl.ds(128 * j, 128)], out_sem.at[T + j])
            cp.start()
            outs.append(cp)

        @pl.loop(1, n_chip)
        def _(i):
            r = 2 * ((chip + n_chip - i) % n_chip) + core
            block_copy(r, partner, 0).wait_recv()
            block_copy(r, partner, n_chip + i).start()

        @pl.loop(0, n_chip)
        def _(i):
            r = 2 * ((chip + n_chip - i) % n_chip) + 1 - core
            block_copy(r, partner, 0).wait_recv()

        for j in range(T // 4):
            cp = pltpu.make_async_copy(GM.at[:, j], o_mid.at[:, :, pl.ds(128 * j, 128)],
                                       out_sem.at[T + T // 2 + j])
            cp.start()
            outs.append(cp)

        @pl.loop(0, n_row // 8)
        def _(i):
            both = [jnp.concatenate(
                [GM[8 * i + r, h, pl.ds(0, 16, stride=2), :] + GM[8 * i + r, h, pl.ds(1, 16, stride=2), :]
                 for r in range(8)], axis=0) for h in range(2)]
            CO[pl.ds(8 * i, 8)] = pool_lanes(jnp.concatenate(both, axis=1)).reshape(8, 16, 128)
        cp = pltpu.make_async_copy(CO, o_coarse, out_sem.at[T + T // 2 + T // 4])
        cp.start()
        outs.append(cp)

        @pl.loop(0, n_chip)
        def _(i):
            block_copy(row, partner, i).wait_send()

        @pl.loop(1, n_chip)
        def _(i):
            block_copy(row, partner, n_chip + i).wait_send()
        for cp, goes, comes in halo:
            @pl.when(goes)
            def _(cp=cp):
                cp.wait_send()
        for cp in outs:
            cp.wait()

    return kernel


def solution(mesh):
    n_row, n_col = mesh.shape["row"], mesh.shape["col"]

    def step(sources, labels):
        hbm = pl.BlockSpec(memory_space=pl.ANY)
        sem = pltpu.SemaphoreType.DMA
        blended, fine, mid, coarse = pl.pallas_call(
            make_kernel(n_row, n_col),
            out_shape=(
                jax.ShapeDtypeStruct((128, 1024), F32),
                jax.ShapeDtypeStruct((64, 512), F32),
                jax.ShapeDtypeStruct((n_row, 32, 256), F32),
                jax.ShapeDtypeStruct((n_row, 16, 128), F32),
            ),
            in_specs=[hbm, hbm],
            out_specs=(hbm, hbm, hbm, hbm),
            scratch_shapes=[
                pltpu.VMEM((3, T + 1, ROWS, 128), F32),
                pltpu.VMEM((T + 1, ROWS, 128), jnp.int32),
                pltpu.VMEM((3, T + 1, ROWS, 128), F32),
                pltpu.VMEM((T, 128, 128), F32),
                pltpu.VMEM((T // 2, 64, 128), F32),
                pltpu.VMEM((n_row, 2, 32, 128), F32),
                pltpu.VMEM((n_row, 16, 128), F32),
                pltpu.VMEM((32, 128), F32),
                pltpu.VMEM((2, 32, 128), F32),
                pltpu.VMEM((4, 3, 8, 128), F32),
                pltpu.VMEM((4, 8, 128), jnp.int32),
                pltpu.VMEM((2, 1, 128), F32),
                pltpu.VMEM((n_row, 1, 128), F32),
                pltpu.VMEM((n_col, 1, 128), F32),
                sem((2 * T,)),
                sem((14,)),
                sem((14,)),
                sem((2,)),
                sem((2,)),
                sem((n_row,)),
                sem((n_row,)),
                sem((T + T // 2 + T // 4 + 1,)),
            ],
            compiler_params=pltpu.CompilerParams(
                collective_id=0, has_side_effects=True, vmem_limit_bytes=48 * 1024 * 1024),
        )(sources, labels)
        return blended, fine, mid.reshape(-1, 256), coarse.reshape(-1, 128)

    return jax.shard_map(
        step,
        mesh=mesh,
        in_specs=(P(None, "row", "col"), P("row", "col")),
        out_specs=(P("row", "col"), P("row", "col"), P(None, "col"), P(None, "col")),
        check_vma=False,
    )
```

```python
import jax
import jax.numpy as jnp
from jax import lax
from jax.experimental import pallas as pl
from jax.experimental.pallas import tpu as pltpu
from jax.sharding import PartitionSpec as P

MESH = pl.DeviceIdType.MESH
F32 = jnp.float32
T = 8
ROWS = 144
X = 4
UNROLL = 4


def two_sum(a, b):
    s = a + b
    t = s - a
    return s, (a - (s - t)) + (b - t)


def dd_add(a, b):
    s, e = two_sum(a[0], b[0])
    return two_sum(s, e + (a[1] + b[1]))


def dd_neg(a):
    return (-a[0], -a[1])


def dd_sub(a, b):
    return dd_add(a, dd_neg(b))


def split(a):
    t = a * 4097.0
    hi = t - (t - a)
    return hi, a - hi


def two_prod(a, b):
    p = a * b
    ah, al = split(a)
    bh, bl = split(b)
    return p, ((ah * bh - p) + ah * bl + al * bh) + al * bl


def dd_mul(a, b):
    p, e = two_prod(a[0], b[0])
    return two_sum(p, e + (a[0] * b[1] + a[1] * b[0]))


def dd_div(a, b):
    q = a[0] / b[0]
    p, e = two_prod(q, b[0])
    r = ((a[0] - p) - e) + (a[1] - q * b[1])
    return two_sum(q, r / b[0])


def krylov_weights(n):
    l1 = dd_div(n[2], n[1])
    l2 = dd_div(n[3], n[1])
    d1 = dd_sub(n[3], dd_mul(l1, n[2]))
    e = dd_sub(n[4], dd_mul(l1, n[3]))
    l3 = dd_div(e, d1)
    d2 = dd_sub(dd_sub(n[5], dd_mul(l2, n[3])), dd_mul(l3, e))
    y1 = dd_sub(n[1], dd_mul(l1, n[0]))
    y2 = dd_sub(dd_sub(n[2], dd_mul(l2, n[0])), dd_mul(l3, y1))
    ok1 = d1[0] > 1e-10 * n[3][0]
    ok2 = ok1 & (d2[0] > 1e-10 * n[5][0])
    c2 = tuple(jnp.where(ok2, v, 0.0) for v in dd_div(y2, d2))
    c1 = dd_sub(dd_div(y1, d1), dd_mul(l3, c2))
    c1 = tuple(jnp.where(ok1, v, 0.0) for v in c1)
    c0 = dd_sub(dd_sub(dd_div(n[0], n[1]), dd_mul(l1, c1)), dd_mul(l2, c2))
    return c0[0], c1[0], c2[0]


def weights(k, step, value, shift=0):
    src = lax.broadcasted_iota(jnp.int32, (k, 128), 0)
    dst = lax.broadcasted_iota(jnp.int32, (k, 128), 1)
    return jnp.where(src // step + shift == dst, value, 0.0).astype(jnp.bfloat16)


def exact_dot(v, weight):
    hi = v.astype(jnp.bfloat16)
    rest = v - hi.astype(F32)
    mid = rest.astype(jnp.bfloat16)
    low = (rest - mid.astype(F32)).astype(jnp.bfloat16)
    dot = lambda p: jnp.dot(p, weight, preferred_element_type=F32)
    return dot(hi) + dot(mid) + dot(low)


def make_kernel(n_row, n_col):
    n_y = n_row // (2 * X)

    def kernel(src, lab, O, FI, H, CO,
               E, L, V, MB, PB, FB, strip, strip_in, corner_in, corner_lab,
               msg, red_row, red_col,
               load_sem, halo_send, halo_recv, red_send, red_recv,
               p_send, p_recv, h_send, h_recv):
        row = lax.axis_index("row")
        col = lax.axis_index("col")
        has_up, has_down = row > 0, row < n_row - 1
        has_left, has_right = col > 0, col < n_col - 1

        loads = []
        for j in (0, T - 1, *range(1, T - 1)):
            lanes = pl.ds(128 * j, 128)
            loads.append(pltpu.make_async_copy(
                src.at[:, :, lanes], E.at[:, j, pl.ds(8, 128), :], load_sem.at[2 * j]))
            loads.append(pltpu.make_async_copy(
                lab.at[:, lanes], L.at[j, pl.ds(8, 128), :], load_sem.at[2 * j + 1]))
        for cp in loads:
            cp.start()

        barrier = pltpu.get_barrier_semaphore()

        @pl.loop(1, n_row)
        def _(i):
            pl.semaphore_signal(barrier, inc=1, device_id={"row": (row + i) % n_row, "col": col},
                                device_id_type=MESH)

        @pl.loop(1, n_col)
        def _(i):
            pl.semaphore_signal(barrier, inc=1, device_id={"row": row, "col": (col + i) % n_col},
                                device_id_type=MESH)

        diagonal = ((-1, -1, has_up & has_left), (-1, 1, has_up & has_right),
                    (1, -1, has_down & has_left), (1, 1, has_down & has_right))
        expected = n_row + n_col - 2
        for dr, dc, there in diagonal:
            @pl.when(there)
            def _(dr=dr, dc=dc):
                pl.semaphore_signal(barrier, inc=1, device_id={"row": row + dr, "col": col + dc},
                                    device_id_type=MESH)
            expected = expected + there.astype(jnp.int32)

        @pl.when(jnp.logical_not(has_up))
        def _():
            E[:, 0:T, 0:8, :] = jnp.zeros((3, T, 8, 128), F32)
            L[0:T, 0:8, :] = jnp.zeros((T, 8, 128), jnp.int32)

        @pl.when(jnp.logical_not(has_down))
        def _():
            E[:, 0:T, 136:144, :] = jnp.zeros((3, T, 8, 128), F32)
            L[0:T, 136:144, :] = jnp.zeros((T, 8, 128), jnp.int32)

        for cp in loads[:4]:
            cp.wait()

        lane = lax.broadcasted_iota(jnp.int32, (128, 128), 1)
        packed = jnp.zeros((128, 128), F32)
        for k in range(4):
            if k < 3:
                first, last = E[k, 0, 8:136, :], E[k, T - 1, 8:136, :]
            else:
                first, last = L[0, 8:136, :].astype(F32), L[T - 1, 8:136, :].astype(F32)
            both = pltpu.roll(jnp.where(lane < 64, first, last), 8 * k + 4, axis=1)
            packed = jnp.where((lane >= 8 * k) & (lane < 8 * k + 8), both, packed)
        strip[...] = packed.T[0:32, :]

        for cp in loads[4:]:
            cp.wait()
        pl.semaphore_wait(barrier, expected)

        def to(r, c):
            return dict(device_id={"row": r, "col": c}, device_id_type=MESH)

        halo = []

        def exchange(slot, s_ref, d_ref, goes, r, c, comes):
            cp = pltpu.make_async_remote_copy(
                src_ref=s_ref, dst_ref=d_ref, send_sem=halo_send.at[slot],
                recv_sem=halo_recv.at[slot], **to(r, c))

            @pl.when(goes)
            def _():
                cp.start()
            halo.append((cp, goes, comes))

        exchange(0, strip, strip_in.at[0], has_right, row, col + 1, has_left)
        exchange(1, strip, strip_in.at[1], has_left, row, col - 1, has_right)
        exchange(2, E.at[:, pl.ds(0, T), pl.ds(8, 8), :], E.at[:, pl.ds(0, T), pl.ds(136, 8), :],
                 has_up, row - 1, col, has_down)
        exchange(3, E.at[:, pl.ds(0, T), pl.ds(128, 8), :], E.at[:, pl.ds(0, T), pl.ds(0, 8), :],
                 has_down, row + 1, col, has_up)
        exchange(4, L.at[pl.ds(0, T), pl.ds(8, 8), :], L.at[pl.ds(0, T), pl.ds(136, 8), :],
                 has_up, row - 1, col, has_down)
        exchange(5, L.at[pl.ds(0, T), pl.ds(128, 8), :], L.at[pl.ds(0, T), pl.ds(0, 8), :],
                 has_down, row + 1, col, has_up)
        slot = 6
        opposite = (diagonal[3][2], diagonal[2][2], diagonal[1][2], diagonal[0][2])
        for q, (dr, dc, there) in enumerate(diagonal):
            rows = pl.ds(8 if dr < 0 else 128, 8)
            j = 0 if dc < 0 else T - 1
            exchange(slot, E.at[:, j, rows, :], corner_in.at[q], there, row + dr, col + dc,
                     opposite[q])
            exchange(slot + 1, L.at[j, rows, :], corner_lab.at[q], there, row + dr, col + dc,
                     opposite[q])
            slot += 2

        for cp, goes, comes in halo:
            @pl.when(comes)
            def _(cp=cp):
                cp.wait_recv()

        sub32 = lax.broadcasted_iota(jnp.int32, (32, 128), 0) % 8
        merged = jnp.where((sub32 < 4) & has_left, strip_in[0],
                           jnp.where((sub32 >= 4) & has_right, strip_in[1], 0.0))
        beside = jnp.concatenate([merged, jnp.zeros((96, 128), F32)], axis=0).T
        outer = (lane < 4) | (lane >= 124)
        for k in range(4):
            tile = jnp.where(outer, pltpu.roll(beside, 128 - (8 * k + 4), axis=1), 0.0)
            if k < 3:
                E[k, T, 8:136, :] = tile
            else:
                L[T, 8:136, :] = tile.astype(jnp.int32)

        lane8 = lax.broadcasted_iota(jnp.int32, (8, 128), 1)
        sub8 = lax.broadcasted_iota(jnp.int32, (8, 128), 0)
        low4, high4 = lane8 < 4, lane8 >= 124
        for rows, from_left, from_right in ((slice(0, 8), 3, 2), (slice(136, 144), 1, 0)):
            l_ok, r_ok = opposite[from_left], opposite[from_right]
            for k in range(3):
                E[k, T, rows, :] = jnp.where(
                    high4 & l_ok, corner_in[from_left, k],
                    jnp.where(low4 & r_ok, corner_in[from_right, k], 0.0))
            L[T, rows, :] = jnp.where(
                high4 & l_ok, corner_lab[from_left],
                jnp.where(low4 & r_ok, corner_lab[from_right], 0))

        col_ok = (low4 & has_right) | (high4 & has_left)
        first_lane, last_lane = lane8 == 0, lane8 == 127

        def stencil(read, rows, rows_up, rows_down, count):
            c = [read(j, rows) for j in range(T + 1)]
            fwd = [pltpu.roll(v, 1, axis=1) for v in c]
            bwd = [pltpu.roll(v, 127, axis=1) for v in c]
            out = []
            for j in range(count):
                left = jnp.where(first_lane, fwd[j - 1], fwd[j])
                right = jnp.where(last_lane, bwd[(j + 1) % (T + 1)], bwd[j])
                near = (read(j, rows_down) + read(j, rows_up)) + (right + left)
                out.append(4.0 * c[j] - near)
            return c, out

        def row_slices(base):
            return pl.ds(base, 8), pl.ds(base - 1, 8), pl.ds(base + 1, 8)

        def store_field(f, rows, tiles, ok):
            for j, v in enumerate(tiles):
                if j == T:
                    v = jnp.where(col_ok, v, 0.0)
                if ok is not None:
                    v = jnp.where(ok, v, 0.0)
                V[f, j, rows, :] = v

        def right_side(base, ok):
            rows, up, down = row_slices(base)
            labels = [L[j, rows, :] for j in range(T + 1)]
            b = [None] * (T + 1)
            for k in range(3):
                _, a = stencil(lambda j, r, k=k: E[k, j, r, :], rows, up, down, T + 1)
                b = a if k == 0 else [
                    jnp.where(lb == k, v, w) for lb, v, w in zip(labels, a, b)]
            store_field(0, rows, b, ok)

        def apply(f, base, ok, count=T + 1):
            rows, up, down = row_slices(base)
            c, a = stencil(lambda j, r: V[f, j, r, :], rows, up, down, count)
            if f < 2:
                store_field(f + 1, rows, a, ok)
            return c, a

        top_ok = has_up | (sub8 == 7)
        bottom_ok = has_down | (sub8 == 0)
        right_side(1, top_ok)
        right_side(135, bottom_ok)

        def body(i, carry):
            right_side(pl.multiple_of(8 * i, 8), None)
            return carry
        lax.fori_loop(1, 17, body, 0, unroll=UNROLL)

        def add_up(products):
            while len(products) > 1:
                products = [a + b for a, b in zip(products[::2], products[1::2])]
            return products[0]

        zero8 = jnp.zeros((8, 128), F32)
        sums = []
        for f in range(3):
            if f < 2:
                apply(f, 1, top_ok)
                apply(f, 135, bottom_ok)

            def body(i, carry, f=f):
                c, a = apply(f, pl.multiple_of(8 * i, 8), None, T + 1 if f < 2 else T)
                same = add_up([c[j] * c[j] for j in range(T)])
                next_ = add_up([c[j] * a[j] for j in range(T)])
                return carry[0] + same, carry[1] + next_
            sums += list(lax.fori_loop(1, 17, body, (zero8, zero8), unroll=UNROLL))

        pairs = [(s, zero8) for s in sums]
        for shift in (4, 2, 1):
            pairs = [dd_add(p, (pltpu.roll(p[0], shift, axis=0), pltpu.roll(p[1], shift, axis=0)))
                     for p in pairs]
        hi, lo = zero8, zero8
        for m, p in enumerate(pairs):
            hi, lo = jnp.where(sub8 == m, p[0], hi), jnp.where(sub8 == m, p[1], lo)
        for shift in (64, 32, 16, 8, 4, 2, 1):
            hi, lo = dd_add((hi, lo), (pltpu.roll(hi, shift, axis=1), pltpu.roll(lo, shift, axis=1)))
        line = jnp.where(lane8 == sub8, hi, 0.0) + jnp.where(lane8 == sub8 + 8, lo, 0.0)
        line = jnp.sum(line, axis=0, keepdims=True)

        lane1 = lax.broadcasted_iota(jnp.int32, (1, 128), 1)

        def total(lines):
            err = []
            while len(lines) > 1:
                both = [two_sum(a, b) for a, b in zip(lines[::2], lines[1::2])]
                lines = [b[0] for b in both]
                err += [b[1] for b in both]
            err = add_up(err + [jnp.zeros((1, 128), F32)])
            low = pltpu.roll(lines[0], 120, axis=1) + err
            h, l = two_sum(lines[0], low)
            return jnp.where(lane1 < 8, h, 0.0) + jnp.where(
                (lane1 >= 8) & (lane1 < 16), pltpu.roll(l, 8, axis=1), 0.0)

        def reduce_start(line, buf, phase, n, me, device):
            msg[phase] = line
            buf[me] = line

            @pl.loop(1, n)
            def _(i):
                pltpu.make_async_remote_copy(
                    src_ref=msg.at[phase], dst_ref=buf.at[me], send_sem=red_send.at[phase],
                    recv_sem=red_recv.at[phase], device_id=device((me + i) % n),
                    device_id_type=MESH).start()

        def reduce_end(buf, phase, n):
            rest = buf.at[pl.ds(0, n - 1)]
            pltpu.make_async_copy(rest, rest, red_recv.at[phase]).wait()
            return total([buf[i] for i in range(n)])

        def reduce_sent(buf, phase, n):
            rest = buf.at[pl.ds(0, n - 1)]
            pltpu.make_async_copy(rest, rest, red_send.at[phase]).wait()

        reduce_start(line, red_col, 0, n_col, col, lambda p: {"row": row, "col": p})

        core, x, y = row % 2, (row // 2) % X, row // (2 * X)
        w4 = weights(512, 4, 1 / 16)
        for h in range(2):
            quads = jnp.concatenate([
                jnp.concatenate([
                    (V[k, 4 * h + j, pl.ds(8, 32, stride=4), :] + V[k, 4 * h + j, pl.ds(9, 32, stride=4), :])
                    + (V[k, 4 * h + j, pl.ds(10, 32, stride=4), :] + V[k, 4 * h + j, pl.ds(11, 32, stride=4), :])
                    for j in range(4)], axis=1) for k in range(3)], axis=0)
            MB[h] = exact_dot(quads, w4).reshape(3, 32, 128)

        def early(h, slot, peer, sem):
            return pltpu.make_async_remote_copy(
                src_ref=MB.at[h], dst_ref=PB.at[slot], send_sem=p_send.at[sem],
                recv_sem=p_recv.at[slot], **to(peer, col))

        early(1 - core, 2 * jnp.where(core == 0, y, x) + core, row + 1 - 2 * core, 0).start()
        for i in range(1, X):
            early(0, 2 * x + core, (y * X + (x + i) % X) * 2, i).start()
        for i in range(1, n_y):
            early(1, 2 * y + core, (((y + i) % n_y) * X + x) * 2 + 1, X - 1 + i).start()
        own_slot = 2 * jnp.where(core == 0, x, y) + core
        PB[own_slot] = MB[core]

        w2 = weights(256, 2, 0.25)
        def fine_part(j):
            pairs2 = jnp.concatenate([
                jnp.concatenate([V[k, 2 * j + h, pl.ds(8, 64, stride=2), :]
                                 + V[k, 2 * j + h, pl.ds(9, 64, stride=2), :] for h in range(2)], axis=1)
                for k in range(3)], axis=0)
            FB[j] = exact_dot(pairs2, w2).reshape(3, 64, 128)

        fine_part(0)
        fine_part(1)
        line = reduce_end(red_col, 0, n_col)
        reduce_start(line, red_row, 1, n_row, row, lambda p: {"row": p, "col": col})
        fine_part(2)
        fine_part(3)
        CO[...] = jnp.zeros((n_y, X, 2, 16, 128), F32)
        reduce_sent(red_col, 0, n_col)

        def early_here(i):
            slot = lax.rem(own_slot + i, 8)
            early(0, slot, row, 0).wait_recv()

        for i in range(1, 8):
            early_here(i)
        line = reduce_end(red_row, 1, n_row)

        pick = lambda m: jnp.sum(jnp.where(lane1 == m, line, 0.0), axis=1, keepdims=True)
        n = [(pick(m), pick(m + 8)) for m in range(6)]
        c0, c1, c2 = (jnp.broadcast_to(c, (8, 128)) for c in krylov_weights(n))

        mine = jnp.where(core == 0, y, x)
        for slot in range(8):
            for r in range(4):
                rows = pl.ds(8 * r, 8)
                H[core, mine, slot // 2, slot % 2, rows, :] = (
                    c0 * PB[slot, 0, rows, :] + c1 * PB[slot, 1, rows, :] + c2 * PB[slot, 2, rows, :])

        def late(h, q, peer, sem):
            return pltpu.make_async_remote_copy(
                src_ref=H.at[h, q], dst_ref=H.at[h, q], send_sem=h_send.at[sem],
                recv_sem=h_recv.at[h, q], **to(peer, col))

        partner = row + 1 - 2 * core
        for i in (2, 1, 3):
            peer = jnp.where(core == 0, (((y + i) % n_y) * X + x) * 2, (y * X + (x + i) % X) * 2 + 1)
            late(core, mine, peer, i).start()
        late(core, mine, partner, 0).start()

        def body(i, carry):
            r = pl.multiple_of(8 * i, 8)
            for j in range(T):
                O[j, pl.ds(r, 8), :] = (
                    c0 * V[0, j, pl.ds(r + 8, 8), :] + c1 * V[1, j, pl.ds(r + 8, 8), :]
                    + c2 * V[2, j, pl.ds(r + 8, 8), :])
            return carry
        lax.fori_loop(0, 16, body, 0, unroll=2)

        def body(i, carry):
            rows = pl.ds(pl.multiple_of(8 * i, 8), 8)
            for j in range(T // 2):
                FI[j, rows, :] = (
                    c0 * FB[j, 0, rows, :] + c1 * FB[j, 1, rows, :] + c2 * FB[j, 2, rows, :])
            return carry
        lax.fori_loop(0, 8, body, 0, unroll=2)

        def coarse(h, q):
            rows = [H[h, q, s // 2, s % 2, pl.ds(0, 16, stride=2), :]
                    + H[h, q, s // 2, s % 2, pl.ds(1, 16, stride=2), :] for s in range(8)]
            out = exact_dot(jnp.concatenate(rows, axis=0), weights(128, 2, 0.25, 64 * h))
            for s in range(8):
                at = (jnp.where(h == 0, q, s // 2), jnp.where(h == 0, s // 2, q), s % 2)
                CO[at] = CO[at] + out[16 * s:16 * s + 16, :]

        coarse(core, mine)
        for i in (1, 3, 2):
            q = (mine + i) % X
            late(core, q, partner, 0).wait_recv()
            late(core, q, partner, X - 1 + i).start()
            coarse(core, q)
        other = 1 - core
        for i in (0, 1, 3, 2):
            q = (jnp.where(core == 0, x, y) + i) % X
            late(other, q, partner, 0).wait_recv()
            coarse(other, q)

        for i in range(7):
            early(0, 0, row, i).wait_send()
        for i in range(7):
            late(0, 0, row, i).wait_send()
        reduce_sent(red_row, 1, n_row)
        for cp, goes, comes in halo:
            @pl.when(goes)
            def _(cp=cp):
                cp.wait_send()

    return kernel


def write_out(O, FI, H, CO, o_blend, o_fine, o_mid, o_coarse, sem):
    copies = [(H.at[0], o_mid.at[:, :, :, :, pl.ds(0, 128)])]
    copies += [(H.at[1, q], o_mid.at[:, q, :, :, pl.ds(128, 128)]) for q in range(X)]
    copies += [(O.at[j], o_blend.at[:, pl.ds(128 * j, 128)]) for j in range(T)]
    copies += [(CO, o_coarse)]
    copies += [(FI.at[j], o_fine.at[:, pl.ds(128 * j, 128)]) for j in range(T // 2)]
    copies = [pltpu.make_async_copy(a, b, sem.at[i]) for i, (a, b) in enumerate(copies)]
    for cp in copies:
        cp.start()
    for cp in copies:
        cp.wait()


def solution(mesh):
    n_row, n_col = mesh.shape["row"], mesh.shape["col"]

    n_y = n_row // (2 * X)

    def step(sources, labels):
        hbm = pl.BlockSpec(memory_space=pltpu.HBM)
        vmem = pl.BlockSpec(memory_space=pltpu.VMEM)
        sem = pltpu.SemaphoreType.DMA
        parts = pl.pallas_call(
            make_kernel(n_row, n_col),
            out_shape=(
                jax.ShapeDtypeStruct((T, 128, 128), F32),
                jax.ShapeDtypeStruct((T // 2, 64, 128), F32),
                jax.ShapeDtypeStruct((2, 4, 4, 2, 32, 128), F32),
                jax.ShapeDtypeStruct((n_y, X, 2, 16, 128), F32),
            ),
            in_specs=[hbm, hbm],
            out_specs=(vmem, vmem, vmem, vmem),
            scratch_shapes=[
                pltpu.VMEM((3, T + 1, ROWS, 128), F32),
                pltpu.VMEM((T + 1, ROWS, 128), jnp.int32),
                pltpu.VMEM((3, T + 1, ROWS, 128), F32),
                pltpu.VMEM((2, 3, 32, 128), F32),
                pltpu.VMEM((8, 3, 32, 128), F32),
                pltpu.VMEM((T // 2, 3, 64, 128), F32),
                pltpu.VMEM((32, 128), F32),
                pltpu.VMEM((2, 32, 128), F32),
                pltpu.VMEM((4, 3, 8, 128), F32),
                pltpu.VMEM((4, 8, 128), jnp.int32),
                pltpu.VMEM((2, 1, 128), F32),
                pltpu.VMEM((n_row, 1, 128), F32),
                pltpu.VMEM((n_col, 1, 128), F32),
                sem((2 * T,)),
                sem((14,)),
                sem((14,)),
                sem((2,)),
                sem((2,)),
                sem((7,)),
                sem((8,)),
                sem((7,)),
                sem((2, 4)),
            ],
            compiler_params=pltpu.CompilerParams(
                collective_id=0, has_side_effects=True, vmem_limit_bytes=40 * 1024 * 1024),
        )(pltpu.with_memory_space_constraint(sources, pltpu.HBM), pltpu.with_memory_space_constraint(labels, pltpu.HBM))
        blended, fine, mid, coarse = pl.pallas_call(
            write_out,
            out_shape=(
                jax.ShapeDtypeStruct((128, 1024), F32),
                jax.ShapeDtypeStruct((64, 512), F32),
                jax.ShapeDtypeStruct((n_y, X, 2, 32, 256), F32),
                jax.ShapeDtypeStruct((n_y, X, 2, 16, 128), F32),
            ),
            in_specs=[vmem] * 4,
            out_specs=(hbm,) * 4,
            scratch_shapes=[sem((5 + T + 1 + T // 2,))],
            compiler_params=pltpu.CompilerParams(vmem_limit_bytes=1024 * 1024),
        )(*parts)
        return blended, fine, mid.reshape(-1, 256), coarse.reshape(-1, 128)

    return jax.shard_map(
        step,
        mesh=mesh,
        in_specs=(P(None, "row", "col"), P("row", "col")),
        out_specs=(P("row", "col"), P("row", "col"), P(None, "col"), P(None, "col")),
        check_vma=False,
    )
```

```python
import jax
import jax.numpy as jnp
from jax import lax
from jax.experimental import pallas as pl
from jax.experimental.pallas import tpu as pltpu
from jax.sharding import PartitionSpec as P

MESH = pl.DeviceIdType.MESH
F32 = jnp.float32
T = 8
ROWS = 144
X = 4
UNROLL = 16
UNROLL_B = 4
UNROLL_C = 8


def two_sum(a, b):
    s = a + b
    t = s - a
    return s, (a - (s - t)) + (b - t)


def dd_add(a, b):
    s, e = two_sum(a[0], b[0])
    return two_sum(s, e + (a[1] + b[1]))


def dd_neg(a):
    return (-a[0], -a[1])


def dd_sub(a, b):
    return dd_add(a, dd_neg(b))


def split(a):
    t = a * 4097.0
    hi = t - (t - a)
    return hi, a - hi


def two_prod(a, b):
    p = a * b
    ah, al = split(a)
    bh, bl = split(b)
    return p, ((ah * bh - p) + ah * bl + al * bh) + al * bl


def dd_mul(a, b):
    p, e = two_prod(a[0], b[0])
    return two_sum(p, e + (a[0] * b[1] + a[1] * b[0]))


def dd_div(a, b):
    q = a[0] / b[0]
    p, e = two_prod(q, b[0])
    r = ((a[0] - p) - e) + (a[1] - q * b[1])
    return two_sum(q, r / b[0])


def krylov_weights(n):
    l1 = dd_div(n[2], n[1])
    l2 = dd_div(n[3], n[1])
    d1 = dd_sub(n[3], dd_mul(l1, n[2]))
    e = dd_sub(n[4], dd_mul(l1, n[3]))
    l3 = dd_div(e, d1)
    d2 = dd_sub(dd_sub(n[5], dd_mul(l2, n[3])), dd_mul(l3, e))
    y1 = dd_sub(n[1], dd_mul(l1, n[0]))
    y2 = dd_sub(dd_sub(n[2], dd_mul(l2, n[0])), dd_mul(l3, y1))
    ok1 = d1[0] > 1e-10 * n[3][0]
    ok2 = ok1 & (d2[0] > 1e-10 * n[5][0])
    c2 = tuple(jnp.where(ok2, v, 0.0) for v in dd_div(y2, d2))
    c1 = dd_sub(dd_div(y1, d1), dd_mul(l3, c2))
    c1 = tuple(jnp.where(ok1, v, 0.0) for v in c1)
    c0 = dd_sub(dd_sub(dd_div(n[0], n[1]), dd_mul(l1, c1)), dd_mul(l2, c2))
    return c0[0], c1[0], c2[0]


def weights(k, step, value, shift=0):
    src = lax.broadcasted_iota(jnp.int32, (k, 128), 0)
    dst = lax.broadcasted_iota(jnp.int32, (k, 128), 1)
    return jnp.where(src // step + shift == dst, value, 0.0).astype(jnp.bfloat16)


def exact_dot(v, weight):
    hi = v.astype(jnp.bfloat16)
    rest = v - hi.astype(F32)
    mid = rest.astype(jnp.bfloat16)
    low = (rest - mid.astype(F32)).astype(jnp.bfloat16)
    dot = lambda p: jnp.dot(p, weight, preferred_element_type=F32)
    return dot(hi) + dot(mid) + dot(low)


def make_kernel(n_row, n_col):
    n_y = n_row // (2 * X)

    def kernel(src, lab, O, FI, H, CO,
               E, L, V, XE, RU, RD, LU, LD, MB, PB, FB, strip, strip_in, corner_in, corner_lab,
               msg, red_row, red_col,
               load_sem, halo_send, halo_recv, red_send, red_recv,
               p_send, p_recv, h_send, h_recv, known):
        row = lax.axis_index("row")
        col = lax.axis_index("col")
        has_up, has_down = row > 0, row < n_row - 1
        has_left, has_right = col > 0, col < n_col - 1

        loads = []
        for j in (0, T - 1, *range(1, T - 1)):
            lanes = pl.ds(128 * j, 128)
            loads.append(pltpu.make_async_copy(
                src.at[:, :, lanes], E.at[:, j, pl.ds(8, 128), :], load_sem.at[2 * j]))
            loads.append(pltpu.make_async_copy(
                lab.at[:, lanes], L.at[j, pl.ds(8, 128), :], load_sem.at[2 * j + 1]))
        for cp in loads:
            cp.start()

        core, x, y = row % 2, (row // 2) % X, row // (2 * X)

        def at(dx=0, dy=0, dcore=0, dcol=0):
            r = (((y + dy) % n_y) * X + (x + dx) % X) * 2 + (core + dcore) % 2
            return {"row": r, "col": (col + dcol) % n_col}

        def signal(sem, device):
            pl.semaphore_signal(sem, inc=1, device_id=device, device_id_type=MESH)

        barrier = pltpu.get_barrier_semaphore()
        beside_us = [at(dcore=1), at(dx=1), at(dx=-1), at(dy=1), at(dy=-1), at(dcol=1), at(dcol=-1)]
        for device in beside_us:
            signal(barrier, device)
        step = 2 * core - 1
        cross = jnp.where(core == 1, has_down, has_up)
        diagonal = ((-1, -1, has_up & has_left), (-1, 1, has_up & has_right),
                    (1, -1, has_down & has_left), (1, 1, has_down & has_right))
        expected = len(beside_us) + cross.astype(jnp.int32)

        @pl.when(cross)
        def _():
            signal(barrier, {"row": row + step, "col": col})
        for dr, dc, there in diagonal:
            @pl.when(there)
            def _(dr=dr, dc=dc):
                signal(barrier, {"row": row + dr, "col": col + dc})
            expected = expected + there.astype(jnp.int32)

        for rows in (slice(0, 8), slice(136, 144)):
            E[:, 0:T, rows, :] = jnp.zeros((3, T, 8, 128), F32)
            L[0:T, rows, :] = jnp.zeros((T, 8, 128), jnp.int32)

        for cp in loads[:4]:
            cp.wait()

        lane = lax.broadcasted_iota(jnp.int32, (128, 128), 1)
        packed = jnp.zeros((128, 128), F32)
        for k in range(4):
            if k < 3:
                first, last = E[k, 0, 8:136, :], E[k, T - 1, 8:136, :]
            else:
                first, last = L[0, 8:136, :].astype(F32), L[T - 1, 8:136, :].astype(F32)
            both = pltpu.roll(jnp.where(lane < 64, first, last), 8 * k + 4, axis=1)
            packed = jnp.where((lane >= 8 * k) & (lane < 8 * k + 8), both, packed)
        strip[...] = packed.T[0:32, :]

        for cp in loads[4:]:
            cp.wait()
        pl.semaphore_wait(barrier, expected)

        def to(r, c):
            return dict(device_id={"row": r, "col": c}, device_id_type=MESH)

        halo = []

        def exchange(slot, s_ref, d_ref, goes, r, c, comes):
            cp = pltpu.make_async_remote_copy(
                src_ref=s_ref, dst_ref=d_ref, send_sem=halo_send.at[slot],
                recv_sem=halo_recv.at[slot], **to(r, c))

            @pl.when(goes)
            def _():
                cp.start()
            halo.append((cp, goes, comes))

        exchange(0, strip, strip_in.at[0], has_right, row, col + 1, has_left)
        exchange(1, strip, strip_in.at[1], has_left, row, col - 1, has_right)
        first4, last4 = pl.ds(8, 4), pl.ds(132, 4)
        exchange(2, E.at[:, pl.ds(0, T), first4, :], RD.at[:, :, pl.ds(0, 4), :],
                 has_up, row - 1, col, has_down)
        exchange(3, E.at[:, pl.ds(0, T), last4, :], RU.at[:, :, pl.ds(4, 4), :],
                 has_down, row + 1, col, has_up)
        exchange(4, L.at[pl.ds(0, T), first4, :], LD.at[:, pl.ds(0, 4), :],
                 has_up, row - 1, col, has_down)
        exchange(5, L.at[pl.ds(0, T), last4, :], LU.at[:, pl.ds(4, 4), :],
                 has_down, row + 1, col, has_up)
        slot = 6
        opposite = (diagonal[3][2], diagonal[2][2], diagonal[1][2], diagonal[0][2])
        for q, (dr, dc, there) in enumerate(diagonal):
            rows = pl.ds(8 if dr < 0 else 128, 8)
            j = 0 if dc < 0 else T - 1
            exchange(slot, E.at[:, j, rows, :], corner_in.at[q], there, row + dr, col + dc,
                     opposite[q])
            exchange(slot + 1, L.at[j, rows, :], corner_lab.at[q], there, row + dr, col + dc,
                     opposite[q])
            slot += 2

        lane8 = lax.broadcasted_iota(jnp.int32, (8, 128), 1)
        sub8 = lax.broadcasted_iota(jnp.int32, (8, 128), 0)
        low4, high4 = lane8 < 4, lane8 >= 124
        col_ok = (low4 & has_right) | (high4 & has_left)
        first_lane, last_lane = lane8 == 0, lane8 == 127

        def stencil(read, rows, rows_up, rows_down, count):
            c = [read(j, rows) for j in range(T + 1)]
            fwd = [pltpu.roll(v, 1, axis=1) for v in c]
            bwd = [pltpu.roll(v, 127, axis=1) for v in c]
            out = []
            for j in range(count):
                left = jnp.where(first_lane, fwd[j - 1], fwd[j])
                right = jnp.where(last_lane, bwd[(j + 1) % (T + 1)], bwd[j])
                near = (read(j, rows_down) + read(j, rows_up)) + (right + left)
                out.append(4.0 * c[j] - near)
            return c, out

        def row_slices(base):
            return pl.ds(base, 8), pl.ds(base - 1, 8), pl.ds(base + 1, 8)

        def store_field(f, rows, tiles, ok):
            for j, v in enumerate(tiles):
                if j == T:
                    v = jnp.where(col_ok, v, 0.0)
                if ok is not None:
                    v = jnp.where(ok, v, 0.0)
                V[f, j, rows, :] = v

        def right_side(base, ok):
            rows, up, down = row_slices(base)
            labels = [L[j, rows, :] for j in range(T + 1)]
            b = [None] * (T + 1)
            for k in range(3):
                _, a = stencil(lambda j, r, k=k: E[k, j, r, :], rows, up, down, T + 1)
                b = a if k == 0 else [
                    jnp.where(lb == k, v, w) for lb, v, w in zip(labels, a, b)]
            store_field(0, rows, b, ok)

        def apply(f, base, ok, count=T + 1):
            rows, up, down = row_slices(base)
            c, a = stencil(lambda j, r: V[f, j, r, :], rows, up, down, count)
            if f < 2:
                store_field(f + 1, rows, a, ok)
            return c, a

        def choose(labels, values):
            return jnp.where(labels == 0, values[0], jnp.where(labels == 1, values[1], values[2]))

        def right_side_alone(base):
            rows, up, down = row_slices(base)
            labels = [L[j, rows, :] for j in range(T)]
            b = None
            for k in range(3):
                c = [E[k, j, rows, :] for j in range(T)]
                fwd = [pltpu.roll(v, 1, axis=1) for v in c]
                bwd = [pltpu.roll(v, 127, axis=1) for v in c]
                XE[k, rows, :] = jnp.where(first_lane, fwd[T - 1], bwd[0])
                a = []
                for j in range(T):
                    left = jnp.where(first_lane, fwd[j - 1] if j else 0.0, fwd[j])
                    right = jnp.where(last_lane, bwd[j + 1] if j < T - 1 else 0.0, bwd[j])
                    near = (E[k, j, down, :] + E[k, j, up, :]) + (right + left)
                    a.append(4.0 * c[j] - near)
                b = a if k == 0 else [jnp.where(lb == k, v, w) for lb, v, w in zip(labels, a, b)]
            for j in range(T):
                V[0, j, rows, :] = b[j]

        def right_side_beside(base):
            rows, up, down = row_slices(base)
            fwd = [pltpu.roll(E[k, T, rows, :], 1, axis=1) for k in range(3)]
            bwd = [pltpu.roll(E[k, T, rows, :], 127, axis=1) for k in range(3)]
            a = []
            for k in range(3):
                left = jnp.where(first_lane, XE[k, rows, :], fwd[k])
                right = jnp.where(last_lane, XE[k, rows, :], bwd[k])
                near = (E[k, T, down, :] + E[k, T, up, :]) + (right + left)
                a.append(4.0 * E[k, T, rows, :] - near)
            V[0, T, rows, :] = jnp.where(col_ok, choose(L[T, rows, :], a), 0.0)
            V[0, 0, rows, :] = V[0, 0, rows, :] - jnp.where(first_lane, choose(L[0, rows, :], fwd), 0.0)
            V[0, T - 1, rows, :] = V[0, T - 1, rows, :] - jnp.where(
                last_lane, choose(L[T - 1, rows, :], bwd), 0.0)

        for device in beside_us:
            signal(known.at[0], device)

        def body(i, carry):
            right_side_alone(pl.multiple_of(8 * i, 8))
            return carry
        lax.fori_loop(1, 17, body, 0, unroll=UNROLL_B)

        pl.semaphore_wait(known.at[0], len(beside_us))
        two_away = [at(dx=2), at(dy=2), at(dcol=2), at(dcol=-2)]
        for device in two_away:
            signal(known.at[1], device)

        for cp, goes, comes in halo:
            @pl.when(comes)
            def _(cp=cp):
                cp.wait_recv()

        sub32 = lax.broadcasted_iota(jnp.int32, (32, 128), 0) % 8
        merged = jnp.where((sub32 < 4) & has_left, strip_in[0],
                           jnp.where((sub32 >= 4) & has_right, strip_in[1], 0.0))
        beside = jnp.concatenate([merged, jnp.zeros((96, 128), F32)], axis=0).T
        outer = (lane < 4) | (lane >= 124)
        for k in range(4):
            tile = jnp.where(outer, pltpu.roll(beside, 128 - (8 * k + 4), axis=1), 0.0)
            if k < 3:
                E[k, T, 8:136, :] = tile
            else:
                L[T, 8:136, :] = tile.astype(jnp.int32)

        for rows, from_left, from_right in ((slice(0, 8), 3, 2), (slice(136, 144), 1, 0)):
            l_ok, r_ok = opposite[from_left], opposite[from_right]
            for k in range(3):
                E[k, T, rows, :] = jnp.where(
                    high4 & l_ok, corner_in[from_left, k],
                    jnp.where(low4 & r_ok, corner_in[from_right, k], 0.0))
            L[T, rows, :] = jnp.where(
                high4 & l_ok, corner_lab[from_left],
                jnp.where(low4 & r_ok, corner_lab[from_right], 0))

        @pl.when(has_up)
        def _():
            for j in range(T):
                for k in range(3):
                    E[k, j, 4:8, :] = RU[k, j, 4:8, :]
                L[j, 4:8, :] = LU[j, 4:8, :]

        @pl.when(has_down)
        def _():
            for j in range(T):
                for k in range(3):
                    E[k, j, 136:140, :] = RD[k, j, 0:4, :]
                L[j, 136:140, :] = LD[j, 0:4, :]

        def body(i, carry):
            right_side_beside(pl.multiple_of(8 * i, 8))
            return carry
        lax.fori_loop(1, 17, body, 0, unroll=UNROLL_C)

        top_ok = has_up | (sub8 == 7)
        bottom_ok = has_down | (sub8 == 0)
        right_side(1, top_ok)
        right_side(135, bottom_ok)

        pl.semaphore_wait(known.at[1], len(two_away))
        signal(known.at[2], at(dcore=1))


        def add_up(products):
            while len(products) > 1:
                products = [a + b for a, b in zip(products[::2], products[1::2])]
            return products[0]

        zero8 = jnp.zeros((8, 128), F32)
        sums = []
        for f in range(3):
            if f < 2:
                apply(f, 1, top_ok)
                apply(f, 135, bottom_ok)

            def body(i, carry, f=f):
                c, a = apply(f, pl.multiple_of(8 * i, 8), None, T + 1 if f < 2 else T)
                same = add_up([c[j] * c[j] for j in range(T)])
                next_ = add_up([c[j] * a[j] for j in range(T)])
                return carry[0] + same, carry[1] + next_
            sums += list(lax.fori_loop(1, 17, body, (zero8, zero8), unroll=UNROLL))

        pairs = [(s, zero8) for s in sums]
        for shift in (4, 2, 1):
            pairs = [dd_add(p, (pltpu.roll(p[0], shift, axis=0), pltpu.roll(p[1], shift, axis=0)))
                     for p in pairs]
        hi, lo = zero8, zero8
        for m, p in enumerate(pairs):
            hi, lo = jnp.where(sub8 == m, p[0], hi), jnp.where(sub8 == m, p[1], lo)
        for shift in (64, 32, 16, 8, 4, 2, 1):
            hi, lo = dd_add((hi, lo), (pltpu.roll(hi, shift, axis=1), pltpu.roll(lo, shift, axis=1)))
        line = jnp.where(lane8 == sub8, hi, 0.0) + jnp.where(lane8 == sub8 + 8, lo, 0.0)
        line = jnp.sum(line, axis=0, keepdims=True)

        lane1 = lax.broadcasted_iota(jnp.int32, (1, 128), 1)

        def total(lines):
            err = []
            while len(lines) > 1:
                both = [two_sum(a, b) for a, b in zip(lines[::2], lines[1::2])]
                lines = [b[0] for b in both]
                err += [b[1] for b in both]
            err = add_up(err + [jnp.zeros((1, 128), F32)])
            low = pltpu.roll(lines[0], 120, axis=1) + err
            h, l = two_sum(lines[0], low)
            return jnp.where(lane1 < 8, h, 0.0) + jnp.where(
                (lane1 >= 8) & (lane1 < 16), pltpu.roll(l, 8, axis=1), 0.0)

        def reduce_start(line, buf, phase, n, me, device):
            msg[phase] = line
            buf[me] = line

            @pl.loop(1, n)
            def _(i):
                pltpu.make_async_remote_copy(
                    src_ref=msg.at[phase], dst_ref=buf.at[me], send_sem=red_send.at[phase],
                    recv_sem=red_recv.at[phase], device_id=device((me + i) % n),
                    device_id_type=MESH).start()

        def reduce_end(buf, phase, n):
            rest = buf.at[pl.ds(0, n - 1)]
            pltpu.make_async_copy(rest, rest, red_recv.at[phase]).wait()
            return total([buf[i] for i in range(n)])

        def reduce_sent(buf, phase, n):
            rest = buf.at[pl.ds(0, n - 1)]
            pltpu.make_async_copy(rest, rest, red_send.at[phase]).wait()

        pl.semaphore_wait(known.at[2], 1)
        reduce_start(line, red_col, 0, n_col, col, lambda p: {"row": row, "col": p})

        w4 = weights(512, 4, 1 / 16)
        for h in range(2):
            quads = jnp.concatenate([
                jnp.concatenate([
                    (V[k, 4 * h + j, pl.ds(8, 32, stride=4), :] + V[k, 4 * h + j, pl.ds(9, 32, stride=4), :])
                    + (V[k, 4 * h + j, pl.ds(10, 32, stride=4), :] + V[k, 4 * h + j, pl.ds(11, 32, stride=4), :])
                    for j in range(4)], axis=1) for k in range(3)], axis=0)
            MB[h] = exact_dot(quads, w4).reshape(3, 32, 128)

        def early(h, slot, peer, sem):
            return pltpu.make_async_remote_copy(
                src_ref=MB.at[h], dst_ref=PB.at[slot], send_sem=p_send.at[sem],
                recv_sem=p_recv.at[slot], **to(peer, col))

        early(1 - core, 2 * jnp.where(core == 0, y, x) + core, row + 1 - 2 * core, 0).start()
        for i in range(1, X):
            early(0, 2 * x + core, (y * X + (x + i) % X) * 2, i).start()
        for i in range(1, n_y):
            early(1, 2 * y + core, (((y + i) % n_y) * X + x) * 2 + 1, X - 1 + i).start()
        own_slot = 2 * jnp.where(core == 0, x, y) + core
        PB[own_slot] = MB[core]

        w2 = weights(256, 2, 0.25)
        def fine_part(j):
            pairs2 = jnp.concatenate([
                jnp.concatenate([V[k, 2 * j + h, pl.ds(8, 64, stride=2), :]
                                 + V[k, 2 * j + h, pl.ds(9, 64, stride=2), :] for h in range(2)], axis=1)
                for k in range(3)], axis=0)
            FB[j] = exact_dot(pairs2, w2).reshape(3, 64, 128)

        fine_part(0)
        fine_part(1)
        line = reduce_end(red_col, 0, n_col)
        reduce_start(line, red_row, 1, n_row, row, lambda p: {"row": p, "col": col})
        fine_part(2)
        fine_part(3)
        CO[...] = jnp.zeros((n_y, X, 2, 16, 128), F32)
        reduce_sent(red_col, 0, n_col)

        def early_here(i):
            slot = lax.rem(own_slot + i, 8)
            early(0, slot, row, 0).wait_recv()

        for i in range(1, 8):
            early_here(i)
        line = reduce_end(red_row, 1, n_row)

        pick = lambda m: jnp.sum(jnp.where(lane1 == m, line, 0.0), axis=1, keepdims=True)
        n = [(pick(m), pick(m + 8)) for m in range(6)]
        c0, c1, c2 = (jnp.broadcast_to(c, (8, 128)) for c in krylov_weights(n))

        mine = jnp.where(core == 0, y, x)
        for slot in range(8):
            for r in range(4):
                rows = pl.ds(8 * r, 8)
                H[core, mine, slot // 2, slot % 2, rows, :] = (
                    c0 * PB[slot, 0, rows, :] + c1 * PB[slot, 1, rows, :] + c2 * PB[slot, 2, rows, :])

        def late(h, q, peer, sem):
            return pltpu.make_async_remote_copy(
                src_ref=H.at[h, q], dst_ref=H.at[h, q], send_sem=h_send.at[sem],
                recv_sem=h_recv.at[h, q], **to(peer, col))

        partner = row + 1 - 2 * core
        for i in (2, 1, 3):
            peer = jnp.where(core == 0, (((y + i) % n_y) * X + x) * 2, (y * X + (x + i) % X) * 2 + 1)
            late(core, mine, peer, i).start()
        late(core, mine, partner, 0).start()

        def body(i, carry):
            r = pl.multiple_of(8 * i, 8)
            for j in range(T):
                O[j, pl.ds(r, 8), :] = (
                    c0 * V[0, j, pl.ds(r + 8, 8), :] + c1 * V[1, j, pl.ds(r + 8, 8), :]
                    + c2 * V[2, j, pl.ds(r + 8, 8), :])
            return carry
        lax.fori_loop(0, 16, body, 0, unroll=2)

        def body(i, carry):
            rows = pl.ds(pl.multiple_of(8 * i, 8), 8)
            for j in range(T // 2):
                FI[j, rows, :] = (
                    c0 * FB[j, 0, rows, :] + c1 * FB[j, 1, rows, :] + c2 * FB[j, 2, rows, :])
            return carry
        lax.fori_loop(0, 8, body, 0, unroll=2)

        def coarse(h, q):
            rows = [H[h, q, s // 2, s % 2, pl.ds(0, 16, stride=2), :]
                    + H[h, q, s // 2, s % 2, pl.ds(1, 16, stride=2), :] for s in range(8)]
            out = exact_dot(jnp.concatenate(rows, axis=0), weights(128, 2, 0.25, 64 * h))
            for s in range(8):
                at = (jnp.where(h == 0, q, s // 2), jnp.where(h == 0, s // 2, q), s % 2)
                CO[at] = CO[at] + out[16 * s:16 * s + 16, :]

        coarse(core, mine)
        for i in (1, 3, 2):
            q = (mine + i) % X
            late(core, q, partner, 0).wait_recv()
            late(core, q, partner, X - 1 + i).start()
        for i in (1, 3, 2):
            coarse(core, (mine + i) % X)
        for i in (0, 1, 3, 2):
            q = (jnp.where(core == 0, x, y) + i) % X
            late(1 - core, q, partner, 0).wait_recv()
            coarse(1 - core, q)

        for i in range(7):
            early(0, 0, row, i).wait_send()
        for i in range(7):
            late(0, 0, row, i).wait_send()
        reduce_sent(red_row, 1, n_row)
        for cp, goes, comes in halo:
            @pl.when(goes)
            def _(cp=cp):
                cp.wait_send()

    return kernel


def write_out(O, FI, H, CO, o_blend, o_fine, o_mid, o_coarse, sem):
    copies = [(H.at[0], o_mid.at[:, :, :, :, pl.ds(0, 128)])]
    copies += [(H.at[1, q], o_mid.at[:, q, :, :, pl.ds(128, 128)]) for q in range(X)]
    copies += [(O.at[j], o_blend.at[:, pl.ds(128 * j, 128)]) for j in range(T)]
    copies += [(CO, o_coarse)]
    copies += [(FI.at[j], o_fine.at[:, pl.ds(128 * j, 128)]) for j in range(T // 2)]
    copies = [pltpu.make_async_copy(a, b, sem.at[i]) for i, (a, b) in enumerate(copies)]
    for cp in copies:
        cp.start()
    for cp in copies:
        cp.wait()


def solution(mesh):
    n_row, n_col = mesh.shape["row"], mesh.shape["col"]

    n_y = n_row // (2 * X)

    def step(sources, labels):
        hbm = pl.BlockSpec(memory_space=pltpu.HBM)
        vmem = pl.BlockSpec(memory_space=pltpu.VMEM)
        sem = pltpu.SemaphoreType.DMA
        parts = pl.pallas_call(
            make_kernel(n_row, n_col),
            out_shape=(
                jax.ShapeDtypeStruct((T, 128, 128), F32),
                jax.ShapeDtypeStruct((T // 2, 64, 128), F32),
                jax.ShapeDtypeStruct((2, 4, 4, 2, 32, 128), F32),
                jax.ShapeDtypeStruct((n_y, X, 2, 16, 128), F32),
            ),
            in_specs=[hbm, hbm],
            out_specs=(vmem, vmem, vmem, vmem),
            scratch_shapes=[
                pltpu.VMEM((3, T + 1, ROWS, 128), F32),
                pltpu.VMEM((T + 1, ROWS, 128), jnp.int32),
                pltpu.VMEM((3, T + 1, ROWS, 128), F32),
                pltpu.VMEM((3, ROWS, 128), F32),
                pltpu.VMEM((3, T, 8, 128), F32),
                pltpu.VMEM((3, T, 8, 128), F32),
                pltpu.VMEM((T, 8, 128), jnp.int32),
                pltpu.VMEM((T, 8, 128), jnp.int32),
                pltpu.VMEM((2, 3, 32, 128), F32),
                pltpu.VMEM((8, 3, 32, 128), F32),
                pltpu.VMEM((T // 2, 3, 64, 128), F32),
                pltpu.VMEM((32, 128), F32),
                pltpu.VMEM((2, 32, 128), F32),
                pltpu.VMEM((4, 3, 8, 128), F32),
                pltpu.VMEM((4, 8, 128), jnp.int32),
                pltpu.VMEM((2, 1, 128), F32),
                pltpu.VMEM((n_row, 1, 128), F32),
                pltpu.VMEM((n_col, 1, 128), F32),
                sem((2 * T,)),
                sem((14,)),
                sem((14,)),
                sem((2,)),
                sem((2,)),
                sem((7,)),
                sem((8,)),
                sem((7,)),
                sem((2, 4)),
                pltpu.SemaphoreType.REGULAR((3,)),
            ],
            compiler_params=pltpu.CompilerParams(
                collective_id=0, has_side_effects=True, vmem_limit_bytes=40 * 1024 * 1024),
        )(pltpu.with_memory_space_constraint(sources, pltpu.HBM), pltpu.with_memory_space_constraint(labels, pltpu.HBM))
        blended, fine, mid, coarse = pl.pallas_call(
            write_out,
            out_shape=(
                jax.ShapeDtypeStruct((128, 1024), F32),
                jax.ShapeDtypeStruct((64, 512), F32),
                jax.ShapeDtypeStruct((n_y, X, 2, 32, 256), F32),
                jax.ShapeDtypeStruct((n_y, X, 2, 16, 128), F32),
            ),
            in_specs=[vmem] * 4,
            out_specs=(hbm,) * 4,
            scratch_shapes=[sem((5 + T + 1 + T // 2,))],
            compiler_params=pltpu.CompilerParams(vmem_limit_bytes=1024 * 1024),
        )(*parts)
        return blended, fine, mid.reshape(-1, 256), coarse.reshape(-1, 128)

    return jax.shard_map(
        step,
        mesh=mesh,
        in_specs=(P(None, "row", "col"), P("row", "col")),
        out_specs=(P("row", "col"), P("row", "col"), P(None, "col"), P(None, "col")),
        check_vma=False,
    )
```

```python
import jax
import jax.numpy as jnp
from jax import lax
from jax.experimental import pallas as pl
from jax.experimental.pallas import tpu as pltpu
from jax.sharding import PartitionSpec as P

MESH = pl.DeviceIdType.MESH
F32 = jnp.float32
T = 8
ROWS = 144
X = 4
UNROLL = 16
UNROLL_B = 4
UNROLL_C = 8


def two_sum(a, b):
    s = a + b
    t = s - a
    return s, (a - (s - t)) + (b - t)


def dd_add(a, b):
    s, e = two_sum(a[0], b[0])
    return two_sum(s, e + (a[1] + b[1]))


def pair_add(a, b):
    s, e = two_sum(a[0], b[0])
    return s, (a[1] + b[1]) + e


def dd_neg(a):
    return (-a[0], -a[1])


def dd_sub(a, b):
    return dd_add(a, dd_neg(b))


def split(a):
    t = a * 4097.0
    hi = t - (t - a)
    return hi, a - hi


def two_prod(a, b):
    p = a * b
    ah, al = split(a)
    bh, bl = split(b)
    return p, ((ah * bh - p) + ah * bl + al * bh) + al * bl


def dd_mul(a, b):
    p, e = two_prod(a[0], b[0])
    return two_sum(p, e + (a[0] * b[1] + a[1] * b[0]))


def dd_div(a, b):
    q = a[0] / b[0]
    p, e = two_prod(q, b[0])
    r = ((a[0] - p) - e) + (a[1] - q * b[1])
    return two_sum(q, r / b[0])


def krylov_weights(n):
    l1 = dd_div(n[2], n[1])
    l2 = dd_div(n[3], n[1])
    d1 = dd_sub(n[3], dd_mul(l1, n[2]))
    e = dd_sub(n[4], dd_mul(l1, n[3]))
    l3 = dd_div(e, d1)
    d2 = dd_sub(dd_sub(n[5], dd_mul(l2, n[3])), dd_mul(l3, e))
    y1 = dd_sub(n[1], dd_mul(l1, n[0]))
    y2 = dd_sub(dd_sub(n[2], dd_mul(l2, n[0])), dd_mul(l3, y1))
    ok1 = d1[0] > 1e-10 * n[3][0]
    ok2 = ok1 & (d2[0] > 1e-10 * n[5][0])
    c2 = tuple(jnp.where(ok2, v, 0.0) for v in dd_div(y2, d2))
    c1 = dd_sub(dd_div(y1, d1), dd_mul(l3, c2))
    c1 = tuple(jnp.where(ok1, v, 0.0) for v in c1)
    c0 = dd_sub(dd_sub(dd_div(n[0], n[1]), dd_mul(l1, c1)), dd_mul(l2, c2))
    return c0[0], c1[0], c2[0]


def weights(k, step, value, shift=0):
    src = lax.broadcasted_iota(jnp.int32, (k, 128), 0)
    dst = lax.broadcasted_iota(jnp.int32, (k, 128), 1)
    return jnp.where(src // step + shift == dst, value, 0.0).astype(jnp.bfloat16)


def exact_dot(v, weight):
    hi = v.astype(jnp.bfloat16)
    rest = v - hi.astype(F32)
    mid = rest.astype(jnp.bfloat16)
    low = (rest - mid.astype(F32)).astype(jnp.bfloat16)
    dot = lambda p: jnp.dot(p, weight, preferred_element_type=F32)
    return dot(hi) + dot(mid) + dot(low)


def make_kernel(n_row, n_col):
    n_y = n_row // (2 * X)

    def kernel(src, lab, O, FI, H, CO,
               E, L, V, XE, RU, RD, LU, LD, MB, PB, FB, strip, strip_in, corner_in, corner_lab,
               msg, red_row, red_col,
               load_sem, halo_send, halo_recv, red_send, red_recv,
               p_send, p_recv, h_send, h_recv, known):
        row = lax.axis_index("row")
        col = lax.axis_index("col")
        has_up, has_down = row > 0, row < n_row - 1
        has_left, has_right = col > 0, col < n_col - 1

        loads = []
        for j in (0, T - 1, *range(1, T - 1)):
            lanes = pl.ds(128 * j, 128)
            loads.append(pltpu.make_async_copy(
                src.at[:, :, lanes], E.at[:, j, pl.ds(8, 128), :], load_sem.at[2 * j]))
            loads.append(pltpu.make_async_copy(
                lab.at[:, lanes], L.at[j, pl.ds(8, 128), :], load_sem.at[2 * j + 1]))
        for cp in loads:
            cp.start()

        core, x, y = row % 2, (row // 2) % X, row // (2 * X)

        def at(dx=0, dy=0, dcore=0, dcol=0):
            r = (((y + dy) % n_y) * X + (x + dx) % X) * 2 + (core + dcore) % 2
            return {"row": r, "col": (col + dcol) % n_col}

        def signal(sem, device):
            pl.semaphore_signal(sem, inc=1, device_id=device, device_id_type=MESH)

        barrier = pltpu.get_barrier_semaphore()
        beside_us = [at(dcore=1), at(dx=1), at(dx=-1), at(dy=1), at(dy=-1), at(dcol=1), at(dcol=-1)]
        for device in beside_us:
            signal(barrier, device)
        step = 2 * core - 1
        cross = jnp.where(core == 1, has_down, has_up)
        diagonal = ((-1, -1, has_up & has_left), (-1, 1, has_up & has_right),
                    (1, -1, has_down & has_left), (1, 1, has_down & has_right))
        expected = len(beside_us) + cross.astype(jnp.int32)

        @pl.when(cross)
        def _():
            signal(barrier, {"row": row + step, "col": col})
        for dr, dc, there in diagonal:
            @pl.when(there)
            def _(dr=dr, dc=dc):
                signal(barrier, {"row": row + dr, "col": col + dc})
            expected = expected + there.astype(jnp.int32)

        for rows in (slice(0, 8), slice(136, 144)):
            E[:, 0:T, rows, :] = jnp.zeros((3, T, 8, 128), F32)
            L[0:T, rows, :] = jnp.zeros((T, 8, 128), jnp.int32)

        for cp in loads[:4]:
            cp.wait()

        lane = lax.broadcasted_iota(jnp.int32, (128, 128), 1)
        packed = jnp.zeros((128, 128), F32)
        for k in range(4):
            if k < 3:
                first, last = E[k, 0, 8:136, :], E[k, T - 1, 8:136, :]
            else:
                first, last = L[0, 8:136, :].astype(F32), L[T - 1, 8:136, :].astype(F32)
            both = pltpu.roll(jnp.where(lane < 64, first, last), 8 * k + 4, axis=1)
            packed = jnp.where((lane >= 8 * k) & (lane < 8 * k + 8), both, packed)
        strip[...] = packed.T[0:32, :]

        for cp in loads[4:]:
            cp.wait()
        pl.semaphore_wait(barrier, expected)

        def to(r, c):
            return dict(device_id={"row": r, "col": c}, device_id_type=MESH)

        for device in beside_us:
            signal(known.at[0], device)


        halo = []

        def exchange(slot, s_ref, d_ref, goes, r, c, comes):
            cp = pltpu.make_async_remote_copy(
                src_ref=s_ref, dst_ref=d_ref, send_sem=halo_send.at[slot],
                recv_sem=halo_recv.at[slot], **to(r, c))

            @pl.when(goes)
            def _():
                cp.start()
            halo.append((cp, goes, comes))

        first4, last4 = pl.ds(8, 4), pl.ds(132, 4)
        exchange(2, E.at[:, pl.ds(0, T), first4, :], RD.at[:, :, pl.ds(0, 4), :],
                 has_up, row - 1, col, has_down)
        exchange(3, E.at[:, pl.ds(0, T), last4, :], RU.at[:, :, pl.ds(4, 4), :],
                 has_down, row + 1, col, has_up)
        exchange(4, L.at[pl.ds(0, T), first4, :], LD.at[:, pl.ds(0, 4), :],
                 has_up, row - 1, col, has_down)
        exchange(5, L.at[pl.ds(0, T), last4, :], LU.at[:, pl.ds(4, 4), :],
                 has_down, row + 1, col, has_up)
        slot = 6
        opposite = (diagonal[3][2], diagonal[2][2], diagonal[1][2], diagonal[0][2])
        for q, (dr, dc, there) in enumerate(diagonal):
            rows, j = pl.ds(8 if dr < 0 else 128, 8), 0 if dc < 0 else T - 1
            exchange(slot, E.at[:, j, rows, :], corner_in.at[q], there, row + dr, col + dc,
                     opposite[q])
            exchange(slot + 1, L.at[j, rows, :], corner_lab.at[q], there, row + dr, col + dc,
                     opposite[q])
            slot += 2

        exchange(0, strip, strip_in.at[0], has_right, row, col + 1, has_left)
        exchange(1, strip, strip_in.at[1], has_left, row, col - 1, has_right)

        lane8 = lax.broadcasted_iota(jnp.int32, (8, 128), 1)
        sub8 = lax.broadcasted_iota(jnp.int32, (8, 128), 0)
        low4, high4 = lane8 < 4, lane8 >= 124
        col_ok = (low4 & has_right) | (high4 & has_left)
        first_lane, last_lane = lane8 == 0, lane8 == 127

        def stencil(read, rows, rows_up, rows_down, count):
            c = [read(j, rows) for j in range(T + 1)]
            fwd = [pltpu.roll(v, 1, axis=1) for v in c]
            bwd = [pltpu.roll(v, 127, axis=1) for v in c]
            out = []
            for j in range(count):
                left = jnp.where(first_lane, fwd[j - 1], fwd[j])
                right = jnp.where(last_lane, bwd[(j + 1) % (T + 1)], bwd[j])
                near = (read(j, rows_down) + read(j, rows_up)) + (right + left)
                out.append(4.0 * c[j] - near)
            return c, out

        def row_slices(base):
            return pl.ds(base, 8), pl.ds(base - 1, 8), pl.ds(base + 1, 8)

        def store_field(f, rows, tiles, ok):
            for j, v in enumerate(tiles):
                if j == T:
                    v = jnp.where(col_ok, v, 0.0)
                if ok is not None:
                    v = jnp.where(ok, v, 0.0)
                V[f, j, rows, :] = v

        def right_side(base, ok):
            rows, up, down = row_slices(base)
            labels = [L[j, rows, :] for j in range(T + 1)]
            b = [None] * (T + 1)
            for k in range(3):
                _, a = stencil(lambda j, r, k=k: E[k, j, r, :], rows, up, down, T + 1)
                b = a if k == 0 else [
                    jnp.where(lb == k, v, w) for lb, v, w in zip(labels, a, b)]
            store_field(0, rows, b, ok)

        def apply(f, base, ok, count=T + 1):
            rows, up, down = row_slices(base)
            c, a = stencil(lambda j, r: V[f, j, r, :], rows, up, down, count)
            if f < 2:
                store_field(f + 1, rows, a, ok)
            return c, a

        def choose(labels, values):
            return jnp.where(labels == 0, values[0], jnp.where(labels == 1, values[1], values[2]))

        def right_side_alone(base):
            rows, up, down = row_slices(base)
            labels = [L[j, rows, :] for j in range(T)]
            b = None
            for k in range(3):
                c = [E[k, j, rows, :] for j in range(T)]
                fwd = [pltpu.roll(v, 1, axis=1) for v in c]
                bwd = [pltpu.roll(v, 127, axis=1) for v in c]
                XE[k, rows, :] = jnp.where(first_lane, fwd[T - 1], bwd[0])
                a = []
                for j in range(T):
                    left = jnp.where(first_lane, fwd[j - 1] if j else 0.0, fwd[j])
                    right = jnp.where(last_lane, bwd[j + 1] if j < T - 1 else 0.0, bwd[j])
                    near = (E[k, j, down, :] + E[k, j, up, :]) + (right + left)
                    a.append(4.0 * c[j] - near)
                b = a if k == 0 else [jnp.where(lb == k, v, w) for lb, v, w in zip(labels, a, b)]
            for j in range(T):
                V[0, j, rows, :] = b[j]

        def right_side_beside(base):
            rows, up, down = row_slices(base)
            fwd = [pltpu.roll(E[k, T, rows, :], 1, axis=1) for k in range(3)]
            bwd = [pltpu.roll(E[k, T, rows, :], 127, axis=1) for k in range(3)]
            a = []
            for k in range(3):
                left = jnp.where(first_lane, XE[k, rows, :], fwd[k])
                right = jnp.where(last_lane, XE[k, rows, :], bwd[k])
                near = (E[k, T, down, :] + E[k, T, up, :]) + (right + left)
                a.append(4.0 * E[k, T, rows, :] - near)
            V[0, T, rows, :] = jnp.where(col_ok, choose(L[T, rows, :], a), 0.0)
            V[0, 0, rows, :] = V[0, 0, rows, :] - jnp.where(first_lane, choose(L[0, rows, :], fwd), 0.0)
            V[0, T - 1, rows, :] = V[0, T - 1, rows, :] - jnp.where(
                last_lane, choose(L[T - 1, rows, :], bwd), 0.0)

        def body(i, carry):
            right_side_alone(pl.multiple_of(8 * i, 8))
            return carry
        lax.fori_loop(1, 9, body, 0, unroll=UNROLL_B)
        pl.semaphore_wait(known.at[0], len(beside_us))
        two_away = [at(dx=2), at(dy=2), at(dcol=2), at(dcol=-2)]
        for device in two_away:
            signal(known.at[1], device)
        lax.fori_loop(9, 17, body, 0, unroll=UNROLL_B)

        def add_up(products):
            while len(products) > 1:
                odd = products[-1:] if len(products) % 2 else []
                products = [a + b for a, b in zip(products[::2], products[1::2])] + odd
            return products[0]

        zero8 = jnp.zeros((8, 128), F32)

        def alone(f, base, inner):
            rows, up, down = row_slices(base)
            c = [V[f, j, rows, :] for j in range(T)]
            fwd = [pltpu.roll(v, 1, axis=1) for v in c]
            bwd = [pltpu.roll(v, 127, axis=1) for v in c]
            a = []
            for j in range(T):
                left = jnp.where(first_lane, fwd[j - 1] if j else 0.0, fwd[j])
                right = jnp.where(last_lane, bwd[j + 1] if j < T - 1 else 0.0, bwd[j])
                near = (V[f, j, down, :] + V[f, j, up, :]) + (right + left)
                a.append(4.0 * c[j] - near)
                if f < 2:
                    V[f + 1, j, rows, :] = a[j]
            if inner:
                return (add_up([c[j] * c[j] for j in range(1, T - 1)]),
                        add_up([c[j] * a[j] for j in range(1, T - 1)]))

        sums = []
        for f in range(3):
            V[f, 0:T, 0:8, :] = jnp.zeros((T, 8, 128), F32)
            V[f, 0:T, 136:144, :] = jnp.zeros((T, 8, 128), F32)
            if f < 2:
                alone(f, 8, False)
                alone(f, 128, False)

            def body(i, carry, f=f):
                got = alone(f, pl.multiple_of(8 * i, 8), True)
                return carry[0] + got[0], carry[1] + got[1]
            sums += list(lax.fori_loop(2, 16, body, (zero8, zero8), unroll=14))

        strips, halo = halo[-2:], halo[:-2]
        for cp, goes, comes in strips:
            @pl.when(comes)
            def _(cp=cp):
                cp.wait_recv()

        sub32 = lax.broadcasted_iota(jnp.int32, (32, 128), 0) % 8
        merged = jnp.where((sub32 < 4) & has_left, strip_in[0],
                           jnp.where((sub32 >= 4) & has_right, strip_in[1], 0.0))
        beside = jnp.concatenate([merged, jnp.zeros((96, 128), F32)], axis=0).T
        outer = (lane < 4) | (lane >= 124)
        for k in range(4):
            tile = jnp.where(outer, pltpu.roll(beside, 128 - (8 * k + 4), axis=1), 0.0)
            if k < 3:
                E[k, T, 8:136, :] = tile
            else:
                L[T, 8:136, :] = tile.astype(jnp.int32)

        def body(i, carry):
            right_side_beside(pl.multiple_of(8 * i, 8))
            return carry
        lax.fori_loop(1, 17, body, 0, unroll=UNROLL_C)

        for cp, goes, comes in halo:
            @pl.when(comes)
            def _(cp=cp):
                cp.wait_recv()

        for rows, from_left, from_right in ((slice(0, 8), 3, 2), (slice(136, 144), 1, 0)):
            l_ok, r_ok = opposite[from_left], opposite[from_right]
            for k in range(3):
                E[k, T, rows, :] = jnp.where(
                    high4 & l_ok, corner_in[from_left, k],
                    jnp.where(low4 & r_ok, corner_in[from_right, k], 0.0))
            L[T, rows, :] = jnp.where(
                high4 & l_ok, corner_lab[from_left],
                jnp.where(low4 & r_ok, corner_lab[from_right], 0))

        @pl.when(has_up)
        def _():
            for j in range(T):
                for k in range(3):
                    E[k, j, 4:8, :] = RU[k, j, 4:8, :]
                L[j, 4:8, :] = LU[j, 4:8, :]

        @pl.when(has_down)
        def _():
            for j in range(T):
                for k in range(3):
                    E[k, j, 136:140, :] = RD[k, j, 0:4, :]
                L[j, 136:140, :] = LD[j, 0:4, :]

        top_ok = has_up | (sub8 == 7)
        bottom_ok = has_down | (sub8 == 0)
        right_side(1, top_ok)
        right_side(135, bottom_ok)

        def rim(f, base):
            rows, up, down = row_slices(base)
            c = {j: V[f, j, rows, :] for j in (T - 2, T - 1, T, 0, 1)}
            fwd = {j: pltpu.roll(c[j], 1, axis=1) for j in (T - 2, T - 1, T, 0)}
            bwd = {j: pltpu.roll(c[j], 127, axis=1) for j in (T - 1, T, 0, 1)}
            a = {}
            for before, j, after in ((T - 2, T - 1, T), (T - 1, T, 0), (T, 0, 1)):
                if j == T and f == 2:
                    continue
                left = jnp.where(first_lane, fwd[before], fwd[j])
                right = jnp.where(last_lane, bwd[after], bwd[j])
                near = (V[f, j, down, :] + V[f, j, up, :]) + (right + left)
                a[j] = 4.0 * c[j] - near
                if f < 2:
                    V[f + 1, j, rows, :] = jnp.where(col_ok, a[j], 0.0) if j == T else a[j]
            return c[0] * c[0] + c[T - 1] * c[T - 1], c[0] * a[0] + c[T - 1] * a[T - 1]

        for f in range(3):
            if f < 2:
                apply(f, 1, top_ok)
                apply(f, 135, bottom_ok)
            same, next_ = sums[2 * f], sums[2 * f + 1]
            for base in (8, 128):
                c, a = apply(f, base, None, T + 1 if f < 2 else T)
                same = same + add_up([c[j] * c[j] for j in range(T)])
                next_ = next_ + add_up([c[j] * a[j] for j in range(T)])

            def body(i, carry, f=f):
                got = rim(f, pl.multiple_of(8 * i, 8))
                return carry[0] + got[0], carry[1] + got[1]
            sums[2 * f:2 * f + 2] = lax.fori_loop(2, 16, body, (same, next_), unroll=14)

        pairs = [(s, zero8) for s in sums]
        for shift in (4, 2, 1):
            pairs = [pair_add(p, (pltpu.roll(p[0], shift, axis=0), pltpu.roll(p[1], shift, axis=0)))
                     for p in pairs]
        hi, lo = zero8, zero8
        for m, p in enumerate(pairs):
            hi, lo = jnp.where(sub8 == m, p[0], hi), jnp.where(sub8 == m, p[1], lo)
        top = hi.astype(jnp.bfloat16).astype(F32)
        mid = (hi - top).astype(jnp.bfloat16).astype(F32)
        low = (hi - top) - mid
        lo_top = lo.astype(jnp.bfloat16).astype(F32)
        pieces = jnp.concatenate([top, mid, low, lo_top, lo - lo_top], axis=0)
        added = jnp.dot(pieces.astype(jnp.bfloat16), jnp.ones((128, 128), jnp.bfloat16),
                        preferred_element_type=F32).reshape(5, 8, 128)
        hi, lo = two_sum(added[0], added[1])
        hi, lo = two_sum(hi, lo + (added[2] + (added[3] + added[4])))
        line = jnp.where(lane8 == sub8, hi, 0.0) + jnp.where(lane8 == sub8 + 8, lo, 0.0)
        line = jnp.sum(line, axis=0, keepdims=True)

        lane1 = lax.broadcasted_iota(jnp.int32, (1, 128), 1)

        def total(lines):
            err = []
            while len(lines) > 1:
                both = [two_sum(a, b) for a, b in zip(lines[::2], lines[1::2])]
                lines = [b[0] for b in both]
                err += [b[1] for b in both]
            err = add_up(err + [jnp.zeros((1, 128), F32)])
            low = pltpu.roll(lines[0], 120, axis=1) + err
            h, l = two_sum(lines[0], low)
            return jnp.where(lane1 < 8, h, 0.0) + jnp.where(
                (lane1 >= 8) & (lane1 < 16), pltpu.roll(l, 8, axis=1), 0.0)

        def reduce_start(line, buf, phase, me, peers):
            msg[phase] = line
            buf[me] = line

            for device in peers:
                pltpu.make_async_remote_copy(
                    src_ref=msg.at[phase], dst_ref=buf.at[me], send_sem=red_send.at[phase],
                    recv_sem=red_recv.at[phase], device_id=device,
                    device_id_type=MESH).start()

        def reduce_end(buf, phase, n):
            rest = buf.at[pl.ds(0, n - 1)]
            pltpu.make_async_copy(rest, rest, red_recv.at[phase]).wait()
            return total([buf[i] for i in range(n)])

        def reduce_sent(buf, phase, n):
            rest = buf.at[pl.ds(0, n - 1)]
            pltpu.make_async_copy(rest, rest, red_send.at[phase]).wait()

        pl.semaphore_wait(known.at[1], len(two_away))
        signal(known.at[2], at(dcore=1))
        reduce_start(line, red_col, 0, col, [
            at(dcol=d) for d in sorted(range(1, n_col), key=lambda d: -min(d, n_col - d))])

        w4 = weights(512, 4, 1 / 16)
        for h in range(2):
            quads = jnp.concatenate([
                jnp.concatenate([
                    (V[k, 4 * h + j, pl.ds(8, 32, stride=4), :] + V[k, 4 * h + j, pl.ds(9, 32, stride=4), :])
                    + (V[k, 4 * h + j, pl.ds(10, 32, stride=4), :] + V[k, 4 * h + j, pl.ds(11, 32, stride=4), :])
                    for j in range(4)], axis=1) for k in range(3)], axis=0)
            MB[h] = exact_dot(quads, w4).reshape(3, 32, 128)

        def early(h, slot, peer, sem):
            return pltpu.make_async_remote_copy(
                src_ref=MB.at[h], dst_ref=PB.at[slot], send_sem=p_send.at[sem],
                recv_sem=p_recv.at[slot], **to(peer, col))

        pl.semaphore_wait(known.at[2], 1)
        early(1 - core, 2 * jnp.where(core == 0, y, x) + core, row + 1 - 2 * core, 0).start()
        for i in range(1, X):
            early(0, 2 * x + core, (y * X + (x + i) % X) * 2, i).start()
        for i in range(1, n_y):
            early(1, 2 * y + core, (((y + i) % n_y) * X + x) * 2 + 1, X - 1 + i).start()
        own_slot = 2 * jnp.where(core == 0, x, y) + core
        PB[own_slot] = MB[core]

        w2 = weights(256, 2, 0.25)
        def fine_part(j):
            pairs2 = jnp.concatenate([
                jnp.concatenate([V[k, 2 * j + h, pl.ds(8, 64, stride=2), :]
                                 + V[k, 2 * j + h, pl.ds(9, 64, stride=2), :] for h in range(2)], axis=1)
                for k in range(3)], axis=0)
            FB[j] = exact_dot(pairs2, w2).reshape(3, 64, 128)

        fine_part(0)
        fine_part(1)
        line = reduce_end(red_col, 0, n_col)
        reduce_start(line, red_row, 1, row, [
            at(dx=dx, dy=dy, dcore=c) for dx, dy, c in sorted(
                [(dx, dy, c) for dx in range(X) for dy in range(n_y) for c in range(2)][1:],
                key=lambda d: -min(d[0], X - d[0]) - min(d[1], n_y - d[1]) - d[2] / 2)])
        fine_part(2)
        fine_part(3)
        CO[...] = jnp.zeros((n_y, X, 2, 16, 128), F32)
        reduce_sent(red_col, 0, n_col)

        def early_here(i):
            slot = lax.rem(own_slot + i, 8)
            early(0, slot, row, 0).wait_recv()

        for i in range(1, 8):
            early_here(i)
        line = reduce_end(red_row, 1, n_row)

        pick = lambda m: jnp.sum(jnp.where(lane1 == m, line, 0.0), axis=1, keepdims=True)
        n = [(pick(m), pick(m + 8)) for m in range(6)]
        c0, c1, c2 = (jnp.broadcast_to(c, (8, 128)) for c in krylov_weights(n))

        mine = jnp.where(core == 0, y, x)
        for slot in range(8):
            for r in range(4):
                rows = pl.ds(8 * r, 8)
                H[core, mine, slot // 2, slot % 2, rows, :] = (
                    c0 * PB[slot, 0, rows, :] + c1 * PB[slot, 1, rows, :] + c2 * PB[slot, 2, rows, :])

        def late(h, q, peer, sem):
            return pltpu.make_async_remote_copy(
                src_ref=H.at[h, q], dst_ref=H.at[h, q], send_sem=h_send.at[sem],
                recv_sem=h_recv.at[h, q], **to(peer, col))

        partner = row + 1 - 2 * core
        for i in (2, 1, 3):
            peer = jnp.where(core == 0, (((y + i) % n_y) * X + x) * 2, (y * X + (x + i) % X) * 2 + 1)
            late(core, mine, peer, i).start()
        late(core, mine, partner, 0).start()

        def body(i, carry):
            r = pl.multiple_of(8 * i, 8)
            for j in range(T):
                O[j, pl.ds(r, 8), :] = (
                    c0 * V[0, j, pl.ds(r + 8, 8), :] + c1 * V[1, j, pl.ds(r + 8, 8), :]
                    + c2 * V[2, j, pl.ds(r + 8, 8), :])
            return carry
        lax.fori_loop(0, 16, body, 0, unroll=2)

        def body(i, carry):
            rows = pl.ds(pl.multiple_of(8 * i, 8), 8)
            for j in range(T // 2):
                FI[j, rows, :] = (
                    c0 * FB[j, 0, rows, :] + c1 * FB[j, 1, rows, :] + c2 * FB[j, 2, rows, :])
            return carry
        lax.fori_loop(0, 8, body, 0, unroll=2)

        def coarse(h, q):
            rows = [H[h, q, s // 2, s % 2, pl.ds(0, 16, stride=2), :]
                    + H[h, q, s // 2, s % 2, pl.ds(1, 16, stride=2), :] for s in range(8)]
            out = exact_dot(jnp.concatenate(rows, axis=0), weights(128, 2, 0.25, 64 * h))
            for s in range(8):
                at = (jnp.where(h == 0, q, s // 2), jnp.where(h == 0, s // 2, q), s % 2)
                CO[at] = CO[at] + out[16 * s:16 * s + 16, :]

        coarse(core, mine)
        for i in (1, 3, 2):
            q = (mine + i) % X
            late(core, q, partner, 0).wait_recv()
            late(core, q, partner, X - 1 + i).start()
        for i in (1, 3, 2):
            coarse(core, (mine + i) % X)
        for i in (0, 1, 3, 2):
            q = (jnp.where(core == 0, x, y) + i) % X
            late(1 - core, q, partner, 0).wait_recv()
            coarse(1 - core, q)

        for i in range(7):
            early(0, 0, row, i).wait_send()
        for i in range(7):
            late(0, 0, row, i).wait_send()
        reduce_sent(red_row, 1, n_row)
        for cp, goes, comes in halo + strips:
            @pl.when(goes)
            def _(cp=cp):
                cp.wait_send()

    return kernel


def write_out(O, FI, H, CO, o_blend, o_fine, o_mid, o_coarse, sem):
    copies = [(H.at[0, q], o_mid.at[q, :, :, :, pl.ds(0, 128)]) for q in range(X)]
    copies += [(H.at[1, q], o_mid.at[:, q, :, :, pl.ds(128, 128)]) for q in range(X)]
    copies += [(O.at[j], o_blend.at[:, pl.ds(128 * j, 128)]) for j in range(T)]
    copies += [(CO.at[q], o_coarse.at[q]) for q in range(CO.shape[0])]
    copies += [(FI.at[j], o_fine.at[:, pl.ds(128 * j, 128)]) for j in range(T // 2)]
    copies = [pltpu.make_async_copy(a, b, sem.at[i]) for i, (a, b) in enumerate(copies)]
    for cp in copies:
        cp.start()
    for cp in copies:
        cp.wait()


def solution(mesh):
    n_row, n_col = mesh.shape["row"], mesh.shape["col"]

    n_y = n_row // (2 * X)

    def step(sources, labels):
        hbm = pl.BlockSpec(memory_space=pltpu.HBM)
        vmem = pl.BlockSpec(memory_space=pltpu.VMEM)
        sem = pltpu.SemaphoreType.DMA
        parts = pl.pallas_call(
            make_kernel(n_row, n_col),
            out_shape=(
                jax.ShapeDtypeStruct((T, 128, 128), F32),
                jax.ShapeDtypeStruct((T // 2, 64, 128), F32),
                jax.ShapeDtypeStruct((2, 4, 4, 2, 32, 128), F32),
                jax.ShapeDtypeStruct((n_y, X, 2, 16, 128), F32),
            ),
            in_specs=[hbm, hbm],
            out_specs=(vmem, vmem, vmem, vmem),
            scratch_shapes=[
                pltpu.VMEM((3, T + 1, ROWS, 128), F32),
                pltpu.VMEM((T + 1, ROWS, 128), jnp.int32),
                pltpu.VMEM((3, T + 1, ROWS, 128), F32),
                pltpu.VMEM((3, ROWS, 128), F32),
                pltpu.VMEM((3, T, 8, 128), F32),
                pltpu.VMEM((3, T, 8, 128), F32),
                pltpu.VMEM((T, 8, 128), jnp.int32),
                pltpu.VMEM((T, 8, 128), jnp.int32),
                pltpu.VMEM((2, 3, 32, 128), F32),
                pltpu.VMEM((8, 3, 32, 128), F32),
                pltpu.VMEM((T // 2, 3, 64, 128), F32),
                pltpu.VMEM((32, 128), F32),
                pltpu.VMEM((2, 32, 128), F32),
                pltpu.VMEM((4, 3, 8, 128), F32),
                pltpu.VMEM((4, 8, 128), jnp.int32),
                pltpu.VMEM((2, 1, 128), F32),
                pltpu.VMEM((n_row, 1, 128), F32),
                pltpu.VMEM((n_col, 1, 128), F32),
                sem((2 * T,)),
                sem((14,)),
                sem((14,)),
                sem((2,)),
                sem((2,)),
                sem((7,)),
                sem((8,)),
                sem((7,)),
                sem((2, 4)),
                pltpu.SemaphoreType.REGULAR((3,)),
            ],
            compiler_params=pltpu.CompilerParams(
                collective_id=0, has_side_effects=True, vmem_limit_bytes=40 * 1024 * 1024),
        )(pltpu.with_memory_space_constraint(sources, pltpu.HBM), pltpu.with_memory_space_constraint(labels, pltpu.HBM))
        blended, fine, mid, coarse = pl.pallas_call(
            write_out,
            out_shape=(
                jax.ShapeDtypeStruct((128, 1024), F32),
                jax.ShapeDtypeStruct((64, 512), F32),
                jax.ShapeDtypeStruct((n_y, X, 2, 32, 256), F32),
                jax.ShapeDtypeStruct((n_y, X, 2, 16, 128), F32),
            ),
            in_specs=[vmem] * 4,
            out_specs=(hbm,) * 4,
            scratch_shapes=[sem((2 * X + T + n_y + T // 2,))],
            compiler_params=pltpu.CompilerParams(vmem_limit_bytes=1024 * 1024),
        )(*parts)
        return blended, fine, mid.reshape(-1, 256), coarse.reshape(-1, 128)

    return jax.shard_map(
        step,
        mesh=mesh,
        in_specs=(P(None, "row", "col"), P("row", "col")),
        out_specs=(P("row", "col"), P("row", "col"), P(None, "col"), P(None, "col")),
        check_vma=False,
    )
```

```python
import jax
import jax.numpy as jnp
from jax import lax
from jax.experimental import pallas as pl
from jax.experimental.pallas import tpu as pltpu
from jax.sharding import PartitionSpec as P

MESH = pl.DeviceIdType.MESH
F32 = jnp.float32
T = 8
ROWS = 144
X = 4
UNROLL = 16
UNROLL_B = 8
UNROLL_C = 16


def two_sum(a, b):
    s = a + b
    t = s - a
    return s, (a - (s - t)) + (b - t)


def dd_add(a, b):
    s, e = two_sum(a[0], b[0])
    return two_sum(s, e + (a[1] + b[1]))


def pair_add(a, b):
    s, e = two_sum(a[0], b[0])
    return s, (a[1] + b[1]) + e


def dd_neg(a):
    return (-a[0], -a[1])


def dd_sub(a, b):
    return dd_add(a, dd_neg(b))


def split(a):
    t = a * 4097.0
    hi = t - (t - a)
    return hi, a - hi


def two_prod(a, b):
    p = a * b
    ah, al = split(a)
    bh, bl = split(b)
    return p, ((ah * bh - p) + ah * bl + al * bh) + al * bl


def dd_mul(a, b):
    p, e = two_prod(a[0], b[0])
    return two_sum(p, e + (a[0] * b[1] + a[1] * b[0]))


def dd_div(a, b):
    q = a[0] / b[0]
    p, e = two_prod(q, b[0])
    r = ((a[0] - p) - e) + (a[1] - q * b[1])
    return two_sum(q, r / b[0])


def krylov_weights(n):
    l1 = dd_div(n[2], n[1])
    l2 = dd_div(n[3], n[1])
    d1 = dd_sub(n[3], dd_mul(l1, n[2]))
    e = dd_sub(n[4], dd_mul(l1, n[3]))
    l3 = dd_div(e, d1)
    d2 = dd_sub(dd_sub(n[5], dd_mul(l2, n[3])), dd_mul(l3, e))
    y1 = dd_sub(n[1], dd_mul(l1, n[0]))
    y2 = dd_sub(dd_sub(n[2], dd_mul(l2, n[0])), dd_mul(l3, y1))
    ok1 = d1[0] > 1e-10 * n[3][0]
    ok2 = ok1 & (d2[0] > 1e-10 * n[5][0])
    c2 = tuple(jnp.where(ok2, v, 0.0) for v in dd_div(y2, d2))
    c1 = dd_sub(dd_div(y1, d1), dd_mul(l3, c2))
    c1 = tuple(jnp.where(ok1, v, 0.0) for v in c1)
    c0 = dd_sub(dd_sub(dd_div(n[0], n[1]), dd_mul(l1, c1)), dd_mul(l2, c2))
    return c0[0], c1[0], c2[0]


def weights(k, step, value, shift=0):
    src = lax.broadcasted_iota(jnp.int32, (k, 128), 0)
    dst = lax.broadcasted_iota(jnp.int32, (k, 128), 1)
    return jnp.where(src // step + shift == dst, value, 0.0).astype(jnp.bfloat16)


def exact_dot(v, weight):
    hi = v.astype(jnp.bfloat16)
    rest = v - hi.astype(F32)
    mid = rest.astype(jnp.bfloat16)
    low = (rest - mid.astype(F32)).astype(jnp.bfloat16)
    dot = lambda p: jnp.dot(p, weight, preferred_element_type=F32)
    return dot(hi) + dot(mid) + dot(low)


def make_kernel(n_row, n_col):
    n_y = n_row // (2 * X)

    def kernel(src, lab, O, FI, H, CO,
               E, L, V, XE, RU, RD, LU, LD, MB, PB, FB, strip, strip_in, corner_in, corner_lab,
               msg, red_row, red_col,
               load_sem, halo_send, halo_recv, red_send, red_recv,
               p_send, p_recv, h_send, h_recv, known):
        row = lax.axis_index("row")
        col = lax.axis_index("col")
        has_up, has_down = row > 0, row < n_row - 1
        has_left, has_right = col > 0, col < n_col - 1

        loads = []
        for j in (0, T - 1, *range(1, T - 1)):
            lanes = pl.ds(128 * j, 128)
            loads.append(pltpu.make_async_copy(
                src.at[:, :, lanes], E.at[:, j, pl.ds(8, 128), :], load_sem.at[2 * j]))
            loads.append(pltpu.make_async_copy(
                lab.at[:, lanes], L.at[j, pl.ds(8, 128), :], load_sem.at[2 * j + 1]))
        for cp in loads:
            cp.start()

        core, x, y = row % 2, (row // 2) % X, row // (2 * X)

        def at(dx=0, dy=0, dcore=0, dcol=0):
            r = (((y + dy) % n_y) * X + (x + dx) % X) * 2 + (core + dcore) % 2
            return {"row": r, "col": (col + dcol) % n_col}

        def signal(sem, device):
            pl.semaphore_signal(sem, inc=1, device_id=device, device_id_type=MESH)

        barrier = pltpu.get_barrier_semaphore()
        beside_us = [at(dcore=1), at(dx=1), at(dx=-1), at(dy=1), at(dy=-1), at(dcol=1), at(dcol=-1)]
        step = 2 * core - 1
        cross = jnp.where(core == 1, has_down, has_up)
        diagonal = ((-1, -1, has_up & has_left), (-1, 1, has_up & has_right),
                    (1, -1, has_down & has_left), (1, 1, has_down & has_right))
        expected = len(beside_us) + cross.astype(jnp.int32)

        for dr, dc, there in diagonal:
            @pl.when(there)
            def _(dr=dr, dc=dc):
                signal(barrier, {"row": row + dr, "col": col + dc})
            expected = expected + there.astype(jnp.int32)
        @pl.when(cross)
        def _():
            signal(barrier, {"row": row + step, "col": col})
        for device in beside_us:
            signal(barrier, device)

        for rows in (slice(0, 8), slice(136, 144)):
            E[:, 0:T, rows, :] = jnp.zeros((3, T, 8, 128), F32)
            L[0:T, rows, :] = jnp.zeros((T, 8, 128), jnp.int32)

        for cp in loads[:4]:
            cp.wait()

        lane = lax.broadcasted_iota(jnp.int32, (128, 128), 1)
        packed = jnp.zeros((128, 128), F32)
        for k in range(4):
            if k < 3:
                first, last = E[k, 0, 8:136, :], E[k, T - 1, 8:136, :]
            else:
                first, last = L[0, 8:136, :].astype(F32), L[T - 1, 8:136, :].astype(F32)
            both = pltpu.roll(jnp.where(lane < 64, first, last), 8 * k + 4, axis=1)
            packed = jnp.where((lane >= 8 * k) & (lane < 8 * k + 8), both, packed)
        strip[...] = packed.T[0:32, :]

        for cp in loads[4:]:
            cp.wait()
        pl.semaphore_wait(barrier, expected)

        def to(r, c):
            return dict(device_id={"row": r, "col": c}, device_id_type=MESH)

        for device in beside_us:
            signal(known.at[0], device)


        halo = []

        def exchange(slot, s_ref, d_ref, goes, r, c, comes):
            cp = pltpu.make_async_remote_copy(
                src_ref=s_ref, dst_ref=d_ref, send_sem=halo_send.at[slot],
                recv_sem=halo_recv.at[slot], **to(r, c))

            @pl.when(goes)
            def _():
                cp.start()
            halo.append((cp, goes, comes))

        exchange(0, strip, strip_in.at[0], has_right, row, col + 1, has_left)
        exchange(1, strip, strip_in.at[1], has_left, row, col - 1, has_right)
        first4, last4 = pl.ds(8, 4), pl.ds(132, 4)
        exchange(2, E.at[:, pl.ds(0, T), first4, :], RD.at[:, :, pl.ds(0, 4), :],
                 has_up, row - 1, col, has_down)
        exchange(3, E.at[:, pl.ds(0, T), last4, :], RU.at[:, :, pl.ds(4, 4), :],
                 has_down, row + 1, col, has_up)
        exchange(4, L.at[pl.ds(0, T), first4, :], LD.at[:, pl.ds(0, 4), :],
                 has_up, row - 1, col, has_down)
        exchange(5, L.at[pl.ds(0, T), last4, :], LU.at[:, pl.ds(4, 4), :],
                 has_down, row + 1, col, has_up)
        slot = 6
        opposite = (diagonal[3][2], diagonal[2][2], diagonal[1][2], diagonal[0][2])
        for q, (dr, dc, there) in enumerate(diagonal):
            rows, j = pl.ds(8 if dr < 0 else 128, 8), 0 if dc < 0 else T - 1
            exchange(slot, E.at[:, j, rows, :], corner_in.at[q], there, row + dr, col + dc,
                     opposite[q])
            exchange(slot + 1, L.at[j, rows, :], corner_lab.at[q], there, row + dr, col + dc,
                     opposite[q])
            slot += 2

        lane8 = lax.broadcasted_iota(jnp.int32, (8, 128), 1)
        sub8 = lax.broadcasted_iota(jnp.int32, (8, 128), 0)
        low4, high4 = lane8 < 4, lane8 >= 124
        col_ok = (low4 & has_right) | (high4 & has_left)
        first_lane, last_lane = lane8 == 0, lane8 == 127

        def stencil(read, rows, rows_up, rows_down, count):
            c = [read(j, rows) for j in range(T + 1)]
            fwd = [pltpu.roll(v, 1, axis=1) for v in c]
            bwd = [pltpu.roll(v, 127, axis=1) for v in c]
            out = []
            for j in range(count):
                left = jnp.where(first_lane, fwd[j - 1], fwd[j])
                right = jnp.where(last_lane, bwd[(j + 1) % (T + 1)], bwd[j])
                near = (read(j, rows_down) + read(j, rows_up)) + (right + left)
                out.append(4.0 * c[j] - near)
            return c, out

        def row_slices(base):
            return pl.ds(base, 8), pl.ds(base - 1, 8), pl.ds(base + 1, 8)

        def store_field(f, rows, tiles, ok):
            for j, v in enumerate(tiles):
                if j == T:
                    v = jnp.where(col_ok, v, 0.0)
                if ok is not None:
                    v = jnp.where(ok, v, 0.0)
                V[f, j, rows, :] = v

        def right_side(base, ok):
            rows, up, down = row_slices(base)
            labels = [L[j, rows, :] for j in range(T + 1)]
            b = [None] * (T + 1)
            for k in range(3):
                _, a = stencil(lambda j, r, k=k: E[k, j, r, :], rows, up, down, T + 1)
                b = a if k == 0 else [
                    jnp.where(lb == k, v, w) for lb, v, w in zip(labels, a, b)]
            store_field(0, rows, b, ok)

        def apply(f, base, ok, count=T + 1):
            rows, up, down = row_slices(base)
            c, a = stencil(lambda j, r: V[f, j, r, :], rows, up, down, count)
            if f < 2:
                store_field(f + 1, rows, a, ok)
            return c, a

        def choose(labels, values):
            return jnp.where(labels == 0, values[0], jnp.where(labels == 1, values[1], values[2]))

        def right_side_alone(base):
            rows, up, down = row_slices(base)
            labels = [L[j, rows, :] for j in range(T)]
            b = None
            for k in range(3):
                c = [E[k, j, rows, :] for j in range(T)]
                fwd = [pltpu.roll(v, 1, axis=1) for v in c]
                bwd = [pltpu.roll(v, 127, axis=1) for v in c]
                XE[k, rows, :] = jnp.where(first_lane, fwd[T - 1], bwd[0])
                a = []
                for j in range(T):
                    left = jnp.where(first_lane, fwd[j - 1] if j else 0.0, fwd[j])
                    right = jnp.where(last_lane, bwd[j + 1] if j < T - 1 else 0.0, bwd[j])
                    near = (E[k, j, down, :] + E[k, j, up, :]) + (right + left)
                    a.append(4.0 * c[j] - near)
                b = a if k == 0 else [jnp.where(lb == k, v, w) for lb, v, w in zip(labels, a, b)]
            for j in range(T):
                V[0, j, rows, :] = b[j]

        def right_side_beside(base):
            rows, up, down = row_slices(base)
            fwd = [pltpu.roll(E[k, T, rows, :], 1, axis=1) for k in range(3)]
            bwd = [pltpu.roll(E[k, T, rows, :], 127, axis=1) for k in range(3)]
            a = []
            for k in range(3):
                left = jnp.where(first_lane, XE[k, rows, :], fwd[k])
                right = jnp.where(last_lane, XE[k, rows, :], bwd[k])
                near = (E[k, T, down, :] + E[k, T, up, :]) + (right + left)
                a.append(4.0 * E[k, T, rows, :] - near)
            V[0, T, rows, :] = jnp.where(col_ok, choose(L[T, rows, :], a), 0.0)
            V[0, 0, rows, :] = V[0, 0, rows, :] - jnp.where(first_lane, choose(L[0, rows, :], fwd), 0.0)
            V[0, T - 1, rows, :] = V[0, T - 1, rows, :] - jnp.where(
                last_lane, choose(L[T - 1, rows, :], bwd), 0.0)

        def body(i, carry):
            right_side_alone(pl.multiple_of(8 * i, 8))
            return carry
        lax.fori_loop(1, 17, body, 0, unroll=UNROLL_B)

        def add_up(products):
            while len(products) > 1:
                odd = products[-1:] if len(products) % 2 else []
                products = [a + b for a, b in zip(products[::2], products[1::2])] + odd
            return products[0]

        zero8 = jnp.zeros((8, 128), F32)

        def alone(f, base, inner):
            rows, up, down = row_slices(base)
            c = [V[f, j, rows, :] for j in range(T)]
            fwd = [pltpu.roll(v, 1, axis=1) for v in c]
            bwd = [pltpu.roll(v, 127, axis=1) for v in c]
            a = []
            for j in range(T):
                left = jnp.where(first_lane, fwd[j - 1] if j else 0.0, fwd[j])
                right = jnp.where(last_lane, bwd[j + 1] if j < T - 1 else 0.0, bwd[j])
                near = (V[f, j, down, :] + V[f, j, up, :]) + (right + left)
                a.append(4.0 * c[j] - near)
                if f < 2:
                    V[f + 1, j, rows, :] = a[j]
            if inner:
                return (add_up([c[j] * c[j] for j in range(1, T - 1)]),
                        add_up([c[j] * a[j] for j in range(1, T - 1)]))

        sums = []
        for f in range(3):
            V[f, 0:T, 0:8, :] = jnp.zeros((T, 8, 128), F32)
            V[f, 0:T, 136:144, :] = jnp.zeros((T, 8, 128), F32)
            if f < 2:
                alone(f, 8, False)
                alone(f, 128, False)

            def body(i, carry, f=f):
                got = alone(f, pl.multiple_of(8 * i, 8), True)
                return carry[0] + got[0], carry[1] + got[1]
            sums += list(lax.fori_loop(2, 16, body, (zero8, zero8), unroll=14))
            if f == 0:
                pl.semaphore_wait(known.at[0], len(beside_us))
                two_away = [at(dx=2), at(dy=2), at(dcol=2), at(dcol=-2)]
                for device in two_away:
                    signal(known.at[1], device)

        strips, halo = halo[:2], halo[2:]
        for cp, goes, comes in strips:
            @pl.when(comes)
            def _(cp=cp):
                cp.wait_recv()

        sub32 = lax.broadcasted_iota(jnp.int32, (32, 128), 0) % 8
        merged = jnp.where((sub32 < 4) & has_left, strip_in[0],
                           jnp.where((sub32 >= 4) & has_right, strip_in[1], 0.0))
        beside = jnp.concatenate([merged, jnp.zeros((96, 128), F32)], axis=0).T
        outer = (lane < 4) | (lane >= 124)
        for k in range(4):
            tile = jnp.where(outer, pltpu.roll(beside, 128 - (8 * k + 4), axis=1), 0.0)
            if k < 3:
                E[k, T, 8:136, :] = tile
            else:
                L[T, 8:136, :] = tile.astype(jnp.int32)

        def body(i, carry):
            right_side_beside(pl.multiple_of(8 * i, 8))
            return carry
        lax.fori_loop(1, 17, body, 0, unroll=UNROLL_C)

        for cp, goes, comes in halo:
            @pl.when(comes)
            def _(cp=cp):
                cp.wait_recv()

        for rows, from_left, from_right in ((slice(0, 8), 3, 2), (slice(136, 144), 1, 0)):
            l_ok, r_ok = opposite[from_left], opposite[from_right]
            for k in range(3):
                E[k, T, rows, :] = jnp.where(
                    high4 & l_ok, corner_in[from_left, k],
                    jnp.where(low4 & r_ok, corner_in[from_right, k], 0.0))
            L[T, rows, :] = jnp.where(
                high4 & l_ok, corner_lab[from_left],
                jnp.where(low4 & r_ok, corner_lab[from_right], 0))

        @pl.when(has_up)
        def _():
            for j in range(T):
                for k in range(3):
                    E[k, j, 4:8, :] = RU[k, j, 4:8, :]
                L[j, 4:8, :] = LU[j, 4:8, :]

        @pl.when(has_down)
        def _():
            for j in range(T):
                for k in range(3):
                    E[k, j, 136:140, :] = RD[k, j, 0:4, :]
                L[j, 136:140, :] = LD[j, 0:4, :]

        top_ok = has_up | (sub8 == 7)
        bottom_ok = has_down | (sub8 == 0)
        right_side(1, top_ok)
        right_side(135, bottom_ok)

        def rim(f, base):
            rows, up, down = row_slices(base)
            c = {j: V[f, j, rows, :] for j in (T - 2, T - 1, T, 0, 1)}
            fwd = {j: pltpu.roll(c[j], 1, axis=1) for j in (T - 2, T - 1, T, 0)}
            bwd = {j: pltpu.roll(c[j], 127, axis=1) for j in (T - 1, T, 0, 1)}
            a = {}
            for before, j, after in ((T - 2, T - 1, T), (T - 1, T, 0), (T, 0, 1)):
                if j == T and f == 2:
                    continue
                left = jnp.where(first_lane, fwd[before], fwd[j])
                right = jnp.where(last_lane, bwd[after], bwd[j])
                near = (V[f, j, down, :] + V[f, j, up, :]) + (right + left)
                a[j] = 4.0 * c[j] - near
                if f < 2:
                    V[f + 1, j, rows, :] = jnp.where(col_ok, a[j], 0.0) if j == T else a[j]
            return c[0] * c[0] + c[T - 1] * c[T - 1], c[0] * a[0] + c[T - 1] * a[T - 1]

        for f in range(3):
            if f < 2:
                apply(f, 1, top_ok)
                apply(f, 135, bottom_ok)
            same, next_ = sums[2 * f], sums[2 * f + 1]
            for base in (8, 128):
                c, a = apply(f, base, None, T + 1 if f < 2 else T)
                same = same + add_up([c[j] * c[j] for j in range(T)])
                next_ = next_ + add_up([c[j] * a[j] for j in range(T)])

            def body(i, carry, f=f):
                got = rim(f, pl.multiple_of(8 * i, 8))
                return carry[0] + got[0], carry[1] + got[1]
            sums[2 * f:2 * f + 2] = lax.fori_loop(2, 16, body, (same, next_), unroll=14)

        pairs = [(s, zero8) for s in sums]
        for shift in (4, 2, 1):
            pairs = [pair_add(p, (pltpu.roll(p[0], shift, axis=0), pltpu.roll(p[1], shift, axis=0)))
                     for p in pairs]
        hi, lo = zero8, zero8
        for m, p in enumerate(pairs):
            hi, lo = jnp.where(sub8 == m, p[0], hi), jnp.where(sub8 == m, p[1], lo)
        top = hi.astype(jnp.bfloat16).astype(F32)
        mid = (hi - top).astype(jnp.bfloat16).astype(F32)
        low = (hi - top) - mid
        lo_top = lo.astype(jnp.bfloat16).astype(F32)
        pieces = jnp.concatenate([top, mid, low, lo_top, lo - lo_top], axis=0)
        added = jnp.dot(pieces.astype(jnp.bfloat16), jnp.ones((128, 128), jnp.bfloat16),
                        preferred_element_type=F32).reshape(5, 8, 128)
        hi, lo = two_sum(added[0], added[1])
        hi, lo = two_sum(hi, lo + (added[2] + (added[3] + added[4])))
        line = jnp.where(lane8 == sub8, hi, 0.0) + jnp.where(lane8 == sub8 + 8, lo, 0.0)
        line = jnp.sum(line, axis=0, keepdims=True)

        lane1 = lax.broadcasted_iota(jnp.int32, (1, 128), 1)

        def total(lines):
            err = []
            while len(lines) > 1:
                both = [two_sum(a, b) for a, b in zip(lines[::2], lines[1::2])]
                lines = [b[0] for b in both]
                err += [b[1] for b in both]
            err = add_up(err + [jnp.zeros((1, 128), F32)])
            low = pltpu.roll(lines[0], 120, axis=1) + err
            h, l = two_sum(lines[0], low)
            return jnp.where(lane1 < 8, h, 0.0) + jnp.where(
                (lane1 >= 8) & (lane1 < 16), pltpu.roll(l, 8, axis=1), 0.0)

        def reduce_start(line, buf, phase, me, peers):
            msg[phase] = line
            buf[me] = line

            for device in peers:
                pltpu.make_async_remote_copy(
                    src_ref=msg.at[phase], dst_ref=buf.at[me], send_sem=red_send.at[phase],
                    recv_sem=red_recv.at[phase], device_id=device,
                    device_id_type=MESH).start()

        def reduce_end(buf, phase, n):
            rest = buf.at[pl.ds(0, n - 1)]
            pltpu.make_async_copy(rest, rest, red_recv.at[phase]).wait()
            return total([buf[i] for i in range(n)])

        def reduce_sent(buf, phase, n):
            rest = buf.at[pl.ds(0, n - 1)]
            pltpu.make_async_copy(rest, rest, red_send.at[phase]).wait()

        pl.semaphore_wait(known.at[1], len(two_away))
        signal(known.at[2], at(dcore=1))
        reduce_start(line, red_col, 0, col, [
            at(dcol=d) for d in sorted(range(1, n_col), key=lambda d: -min(d, n_col - d))])

        w4 = weights(512, 4, 1 / 16)
        for h in range(2):
            quads = jnp.concatenate([
                jnp.concatenate([
                    (V[k, 4 * h + j, pl.ds(8, 32, stride=4), :] + V[k, 4 * h + j, pl.ds(9, 32, stride=4), :])
                    + (V[k, 4 * h + j, pl.ds(10, 32, stride=4), :] + V[k, 4 * h + j, pl.ds(11, 32, stride=4), :])
                    for j in range(4)], axis=1) for k in range(3)], axis=0)
            MB[h] = exact_dot(quads, w4).reshape(3, 32, 128)

        def early(h, slot, peer, sem):
            return pltpu.make_async_remote_copy(
                src_ref=MB.at[h], dst_ref=PB.at[slot], send_sem=p_send.at[sem],
                recv_sem=p_recv.at[slot], **to(peer, col))

        pl.semaphore_wait(known.at[2], 1)
        early(1 - core, 2 * jnp.where(core == 0, y, x) + core, row + 1 - 2 * core, 0).start()
        for i in range(1, X):
            early(0, 2 * x + core, (y * X + (x + i) % X) * 2, i).start()
        for i in range(1, n_y):
            early(1, 2 * y + core, (((y + i) % n_y) * X + x) * 2 + 1, X - 1 + i).start()
        own_slot = 2 * jnp.where(core == 0, x, y) + core
        PB[own_slot] = MB[core]

        w2 = weights(256, 2, 0.25)
        def fine_part(j):
            pairs2 = jnp.concatenate([
                jnp.concatenate([V[k, 2 * j + h, pl.ds(8, 64, stride=2), :]
                                 + V[k, 2 * j + h, pl.ds(9, 64, stride=2), :] for h in range(2)], axis=1)
                for k in range(3)], axis=0)
            FB[j] = exact_dot(pairs2, w2).reshape(3, 64, 128)

        fine_part(0)
        fine_part(1)
        line = reduce_end(red_col, 0, n_col)
        reduce_start(line, red_row, 1, row, [
            at(dx=dx, dy=dy, dcore=c) for dx, dy, c in sorted(
                [(dx, dy, c) for dx in range(X) for dy in range(n_y) for c in range(2)][1:],
                key=lambda d: -min(d[0], X - d[0]) - min(d[1], n_y - d[1]) - d[2] / 2)])
        fine_part(2)
        fine_part(3)
        CO[...] = jnp.zeros((n_y, X, 2, 16, 128), F32)
        reduce_sent(red_col, 0, n_col)

        def early_here(i):
            slot = lax.rem(own_slot + i, 8)
            early(0, slot, row, 0).wait_recv()

        for i in range(1, 8):
            early_here(i)
        line = reduce_end(red_row, 1, n_row)

        pick = lambda m: jnp.sum(jnp.where(lane1 == m, line, 0.0), axis=1, keepdims=True)
        n = [(pick(m), pick(m + 8)) for m in range(6)]
        c0, c1, c2 = (jnp.broadcast_to(c, (8, 128)) for c in krylov_weights(n))

        mine = jnp.where(core == 0, y, x)
        for slot in range(8):
            for r in range(4):
                rows = pl.ds(8 * r, 8)
                H[core, mine, slot // 2, slot % 2, rows, :] = (
                    c0 * PB[slot, 0, rows, :] + c1 * PB[slot, 1, rows, :] + c2 * PB[slot, 2, rows, :])

        def late(h, q, peer, sem):
            return pltpu.make_async_remote_copy(
                src_ref=H.at[h, q], dst_ref=H.at[h, q], send_sem=h_send.at[sem],
                recv_sem=h_recv.at[h, q], **to(peer, col))

        partner = row + 1 - 2 * core
        for i in (2, 1, 3):
            peer = jnp.where(core == 0, (((y + i) % n_y) * X + x) * 2, (y * X + (x + i) % X) * 2 + 1)
            late(core, mine, peer, i).start()
        late(core, mine, partner, 0).start()

        def body(i, carry):
            r = pl.multiple_of(8 * i, 8)
            for j in range(T):
                O[j, pl.ds(r, 8), :] = (
                    c0 * V[0, j, pl.ds(r + 8, 8), :] + c1 * V[1, j, pl.ds(r + 8, 8), :]
                    + c2 * V[2, j, pl.ds(r + 8, 8), :])
            return carry
        lax.fori_loop(0, 16, body, 0, unroll=2)

        def body(i, carry):
            rows = pl.ds(pl.multiple_of(8 * i, 8), 8)
            for j in range(T // 2):
                FI[j, rows, :] = (
                    c0 * FB[j, 0, rows, :] + c1 * FB[j, 1, rows, :] + c2 * FB[j, 2, rows, :])
            return carry
        lax.fori_loop(0, 8, body, 0, unroll=2)

        def coarse(h, q):
            rows = [H[h, q, s // 2, s % 2, pl.ds(0, 16, stride=2), :]
                    + H[h, q, s // 2, s % 2, pl.ds(1, 16, stride=2), :] for s in range(8)]
            out = exact_dot(jnp.concatenate(rows, axis=0), weights(128, 2, 0.25, 64 * h))
            for s in range(8):
                at = (jnp.where(h == 0, q, s // 2), jnp.where(h == 0, s // 2, q), s % 2)
                CO[at] = CO[at] + out[16 * s:16 * s + 16, :]

        coarse(core, mine)
        for i in (1, 3, 2):
            q = (mine + i) % X
            late(core, q, partner, 0).wait_recv()
            late(core, q, partner, X - 1 + i).start()
        for i in (1, 3, 2):
            coarse(core, (mine + i) % X)
        for i in (0, 1, 3, 2):
            q = (jnp.where(core == 0, x, y) + i) % X
            late(1 - core, q, partner, 0).wait_recv()
            coarse(1 - core, q)

        for i in range(7):
            early(0, 0, row, i).wait_send()
        for i in range(7):
            late(0, 0, row, i).wait_send()
        reduce_sent(red_row, 1, n_row)
        for cp, goes, comes in halo + strips:
            @pl.when(goes)
            def _(cp=cp):
                cp.wait_send()

    return kernel


def write_out(O, FI, H, CO, o_blend, o_fine, o_mid, o_coarse, sem):
    copies = [(H.at[0, q], o_mid.at[q, :, :, :, pl.ds(0, 128)]) for q in range(X)]
    copies += [(H.at[1, q], o_mid.at[:, q, :, :, pl.ds(128, 128)]) for q in range(X)]
    copies += [(O.at[j], o_blend.at[:, pl.ds(128 * j, 128)]) for j in range(T)]
    copies += [(CO.at[q], o_coarse.at[q]) for q in range(CO.shape[0])]
    copies += [(FI.at[j], o_fine.at[:, pl.ds(128 * j, 128)]) for j in range(T // 2)]
    copies = [pltpu.make_async_copy(a, b, sem.at[i]) for i, (a, b) in enumerate(copies)]
    for cp in copies:
        cp.start()
    for cp in copies:
        cp.wait()


def solution(mesh):
    n_row, n_col = mesh.shape["row"], mesh.shape["col"]

    n_y = n_row // (2 * X)

    def step(sources, labels):
        hbm = pl.BlockSpec(memory_space=pltpu.HBM)
        vmem = pl.BlockSpec(memory_space=pltpu.VMEM)
        sem = pltpu.SemaphoreType.DMA
        parts = pl.pallas_call(
            make_kernel(n_row, n_col),
            out_shape=(
                jax.ShapeDtypeStruct((T, 128, 128), F32),
                jax.ShapeDtypeStruct((T // 2, 64, 128), F32),
                jax.ShapeDtypeStruct((2, 4, 4, 2, 32, 128), F32),
                jax.ShapeDtypeStruct((n_y, X, 2, 16, 128), F32),
            ),
            in_specs=[hbm, hbm],
            out_specs=(vmem, vmem, vmem, vmem),
            scratch_shapes=[
                pltpu.VMEM((3, T + 1, ROWS, 128), F32),
                pltpu.VMEM((T + 1, ROWS, 128), jnp.int32),
                pltpu.VMEM((3, T + 1, ROWS, 128), F32),
                pltpu.VMEM((3, ROWS, 128), F32),
                pltpu.VMEM((3, T, 8, 128), F32),
                pltpu.VMEM((3, T, 8, 128), F32),
                pltpu.VMEM((T, 8, 128), jnp.int32),
                pltpu.VMEM((T, 8, 128), jnp.int32),
                pltpu.VMEM((2, 3, 32, 128), F32),
                pltpu.VMEM((8, 3, 32, 128), F32),
                pltpu.VMEM((T // 2, 3, 64, 128), F32),
                pltpu.VMEM((32, 128), F32),
                pltpu.VMEM((2, 32, 128), F32),
                pltpu.VMEM((4, 3, 8, 128), F32),
                pltpu.VMEM((4, 8, 128), jnp.int32),
                pltpu.VMEM((2, 1, 128), F32),
                pltpu.VMEM((n_row, 1, 128), F32),
                pltpu.VMEM((n_col, 1, 128), F32),
                sem((2 * T,)),
                sem((14,)),
                sem((14,)),
                sem((2,)),
                sem((2,)),
                sem((7,)),
                sem((8,)),
                sem((7,)),
                sem((2, 4)),
                pltpu.SemaphoreType.REGULAR((3,)),
            ],
            compiler_params=pltpu.CompilerParams(
                collective_id=0, has_side_effects=True, vmem_limit_bytes=40 * 1024 * 1024),
        )(pltpu.with_memory_space_constraint(sources, pltpu.HBM), pltpu.with_memory_space_constraint(labels, pltpu.HBM))
        blended, fine, mid, coarse = pl.pallas_call(
            write_out,
            out_shape=(
                jax.ShapeDtypeStruct((128, 1024), F32),
                jax.ShapeDtypeStruct((64, 512), F32),
                jax.ShapeDtypeStruct((n_y, X, 2, 32, 256), F32),
                jax.ShapeDtypeStruct((n_y, X, 2, 16, 128), F32),
            ),
            in_specs=[vmem] * 4,
            out_specs=(hbm,) * 4,
            scratch_shapes=[sem((2 * X + T + n_y + T // 2,))],
            compiler_params=pltpu.CompilerParams(vmem_limit_bytes=1024 * 1024),
        )(*parts)
        return blended, fine, mid.reshape(-1, 256), coarse.reshape(-1, 128)

    return jax.shard_map(
        step,
        mesh=mesh,
        in_specs=(P(None, "row", "col"), P("row", "col")),
        out_specs=(P("row", "col"), P("row", "col"), P(None, "col"), P(None, "col")),
        check_vma=False,
    )
```

```python
import jax
import jax.numpy as jnp
from jax import lax
from jax.experimental import pallas as pl
from jax.experimental.pallas import tpu as pltpu
from jax.sharding import PartitionSpec as P

MESH = pl.DeviceIdType.MESH
F32 = jnp.float32
T = 8
ROWS = 144
X = 4
UNROLL = 16
UNROLL_B = 8
UNROLL_C = 16


def two_sum(a, b):
    s = a + b
    t = s - a
    return s, (a - (s - t)) + (b - t)


def dd_add(a, b):
    s, e = two_sum(a[0], b[0])
    return two_sum(s, e + (a[1] + b[1]))


def pair_add(a, b):
    s, e = two_sum(a[0], b[0])
    return s, (a[1] + b[1]) + e


def dd_neg(a):
    return (-a[0], -a[1])


def dd_sub(a, b):
    return dd_add(a, dd_neg(b))


def split(a):
    t = a * 4097.0
    hi = t - (t - a)
    return hi, a - hi


def two_prod(a, b):
    p = a * b
    ah, al = split(a)
    bh, bl = split(b)
    return p, ((ah * bh - p) + ah * bl + al * bh) + al * bl


def dd_mul(a, b):
    p, e = two_prod(a[0], b[0])
    return two_sum(p, e + (a[0] * b[1] + a[1] * b[0]))


def dd_div(a, b):
    q = a[0] / b[0]
    p, e = two_prod(q, b[0])
    r = ((a[0] - p) - e) + (a[1] - q * b[1])
    return two_sum(q, r / b[0])


def krylov_weights(n):
    l1 = dd_div(n[2], n[1])
    l2 = dd_div(n[3], n[1])
    d1 = dd_sub(n[3], dd_mul(l1, n[2]))
    e = dd_sub(n[4], dd_mul(l1, n[3]))
    l3 = dd_div(e, d1)
    d2 = dd_sub(dd_sub(n[5], dd_mul(l2, n[3])), dd_mul(l3, e))
    y1 = dd_sub(n[1], dd_mul(l1, n[0]))
    y2 = dd_sub(dd_sub(n[2], dd_mul(l2, n[0])), dd_mul(l3, y1))
    ok1 = d1[0] > 1e-10 * n[3][0]
    ok2 = ok1 & (d2[0] > 1e-10 * n[5][0])
    c2 = tuple(jnp.where(ok2, v, 0.0) for v in dd_div(y2, d2))
    c1 = dd_sub(dd_div(y1, d1), dd_mul(l3, c2))
    c1 = tuple(jnp.where(ok1, v, 0.0) for v in c1)
    c0 = dd_sub(dd_sub(dd_div(n[0], n[1]), dd_mul(l1, c1)), dd_mul(l2, c2))
    return c0[0], c1[0], c2[0]


def weights(k, step, value, shift=0):
    src = lax.broadcasted_iota(jnp.int32, (k, 128), 0)
    dst = lax.broadcasted_iota(jnp.int32, (k, 128), 1)
    return jnp.where(src // step + shift == dst, value, 0.0).astype(jnp.bfloat16)


def exact_dot(v, weight):
    hi = v.astype(jnp.bfloat16)
    rest = v - hi.astype(F32)
    mid = rest.astype(jnp.bfloat16)
    low = (rest - mid.astype(F32)).astype(jnp.bfloat16)
    dot = lambda p: jnp.dot(p, weight, preferred_element_type=F32)
    return dot(hi) + dot(mid) + dot(low)


def make_kernel(n_row, n_col):
    n_y = n_row // (2 * X)

    def kernel(src, lab, O, FI, H, CO,
               E, L, V, XE, RU, RD, LU, LD, MB, PB, FB, strip, strip_in, corner_in, corner_lab,
               msg, red_row, red_col,
               load_sem, halo_send, halo_recv, red_send, red_recv,
               p_send, p_recv, h_send, h_recv, known):
        row = lax.axis_index("row")
        col = lax.axis_index("col")
        has_up, has_down = row > 0, row < n_row - 1
        has_left, has_right = col > 0, col < n_col - 1

        loads = []
        for j in (0, T - 1, *range(1, T - 1)):
            lanes = pl.ds(128 * j, 128)
            loads.append(pltpu.make_async_copy(
                src.at[:, :, lanes], E.at[:, j, pl.ds(8, 128), :], load_sem.at[2 * j]))
            loads.append(pltpu.make_async_copy(
                lab.at[:, lanes], L.at[j, pl.ds(8, 128), :], load_sem.at[2 * j + 1]))
        for cp in loads:
            cp.start()

        core, x, y = row % 2, (row // 2) % X, row // (2 * X)

        def at(dx=0, dy=0, dcore=0, dcol=0):
            r = (((y + dy) % n_y) * X + (x + dx) % X) * 2 + (core + dcore) % 2
            return {"row": r, "col": (col + dcol) % n_col}

        def signal(sem, device):
            pl.semaphore_signal(sem, inc=1, device_id=device, device_id_type=MESH)

        barrier = pltpu.get_barrier_semaphore()
        beside_us = [at(dcore=1), at(dx=1), at(dx=-1), at(dy=1), at(dy=-1), at(dcol=1), at(dcol=-1)]
        step = 2 * core - 1
        cross = jnp.where(core == 1, has_down, has_up)
        diagonal = ((-1, -1, has_up & has_left), (-1, 1, has_up & has_right),
                    (1, -1, has_down & has_left), (1, 1, has_down & has_right))
        expected = len(beside_us) + cross.astype(jnp.int32)

        for dr, dc, there in diagonal:
            @pl.when(there)
            def _(dr=dr, dc=dc):
                signal(barrier, {"row": row + dr, "col": col + dc})
            expected = expected + there.astype(jnp.int32)
        @pl.when(cross)
        def _():
            signal(barrier, {"row": row + step, "col": col})
        for device in beside_us:
            signal(barrier, device)

        for rows in (slice(0, 8), slice(136, 144)):
            E[:, 0:T, rows, :] = jnp.zeros((3, T, 8, 128), F32)
            L[0:T, rows, :] = jnp.zeros((T, 8, 128), jnp.int32)

        for cp in loads[:4]:
            cp.wait()

        lane = lax.broadcasted_iota(jnp.int32, (128, 128), 1)
        packed = jnp.zeros((128, 128), F32)
        for k in range(4):
            if k < 3:
                first, last = E[k, 0, 8:136, :], E[k, T - 1, 8:136, :]
            else:
                first, last = L[0, 8:136, :].astype(F32), L[T - 1, 8:136, :].astype(F32)
            both = pltpu.roll(jnp.where(lane < 64, first, last), 8 * k + 4, axis=1)
            packed = jnp.where((lane >= 8 * k) & (lane < 8 * k + 8), both, packed)
        strip[...] = packed.T[0:32, :]

        for cp in loads[4:]:
            cp.wait()
        pl.semaphore_wait(barrier, expected)

        def to(r, c):
            return dict(device_id={"row": r, "col": c}, device_id_type=MESH)

        for device in beside_us:
            signal(known.at[0], device)


        halo = []

        def exchange(slot, s_ref, d_ref, goes, r, c, comes):
            cp = pltpu.make_async_remote_copy(
                src_ref=s_ref, dst_ref=d_ref, send_sem=halo_send.at[slot],
                recv_sem=halo_recv.at[slot], **to(r, c))

            @pl.when(goes)
            def _():
                cp.start()
            halo.append((cp, goes, comes))

        exchange(0, strip, strip_in.at[0], has_right, row, col + 1, has_left)
        exchange(1, strip, strip_in.at[1], has_left, row, col - 1, has_right)
        first4, last4 = pl.ds(8, 4), pl.ds(132, 4)
        exchange(2, E.at[:, pl.ds(0, T), first4, :], RD.at[:, :, pl.ds(0, 4), :],
                 has_up, row - 1, col, has_down)
        exchange(3, E.at[:, pl.ds(0, T), last4, :], RU.at[:, :, pl.ds(4, 4), :],
                 has_down, row + 1, col, has_up)
        exchange(4, L.at[pl.ds(0, T), first4, :], LD.at[:, pl.ds(0, 4), :],
                 has_up, row - 1, col, has_down)
        exchange(5, L.at[pl.ds(0, T), last4, :], LU.at[:, pl.ds(4, 4), :],
                 has_down, row + 1, col, has_up)
        slot = 6
        opposite = (diagonal[3][2], diagonal[2][2], diagonal[1][2], diagonal[0][2])
        for q, (dr, dc, there) in enumerate(diagonal):
            rows, j = pl.ds(8 if dr < 0 else 128, 8), 0 if dc < 0 else T - 1
            exchange(slot, E.at[:, j, rows, :], corner_in.at[q], there, row + dr, col + dc,
                     opposite[q])
            exchange(slot + 1, L.at[j, rows, :], corner_lab.at[q], there, row + dr, col + dc,
                     opposite[q])
            slot += 2

        lane8 = lax.broadcasted_iota(jnp.int32, (8, 128), 1)
        sub8 = lax.broadcasted_iota(jnp.int32, (8, 128), 0)
        low4, high4 = lane8 < 4, lane8 >= 124
        col_ok = (low4 & has_right) | (high4 & has_left)
        first_lane, last_lane = lane8 == 0, lane8 == 127

        def stencil(read, rows, rows_up, rows_down, count):
            c = [read(j, rows) for j in range(T + 1)]
            fwd = [pltpu.roll(v, 1, axis=1) for v in c]
            bwd = [pltpu.roll(v, 127, axis=1) for v in c]
            out = []
            for j in range(count):
                left = jnp.where(first_lane, fwd[j - 1], fwd[j])
                right = jnp.where(last_lane, bwd[(j + 1) % (T + 1)], bwd[j])
                near = (read(j, rows_down) + read(j, rows_up)) + (right + left)
                out.append(4.0 * c[j] - near)
            return c, out

        def row_slices(base):
            return pl.ds(base, 8), pl.ds(base - 1, 8), pl.ds(base + 1, 8)

        def store_field(f, rows, tiles, ok):
            for j, v in enumerate(tiles):
                if j == T:
                    v = jnp.where(col_ok, v, 0.0)
                if ok is not None:
                    v = jnp.where(ok, v, 0.0)
                V[f, j, rows, :] = v

        def right_side(base, ok):
            rows, up, down = row_slices(base)
            labels = [L[j, rows, :] for j in range(T + 1)]
            b = [None] * (T + 1)
            for k in range(3):
                _, a = stencil(lambda j, r, k=k: E[k, j, r, :], rows, up, down, T + 1)
                b = a if k == 0 else [
                    jnp.where(lb == k, v, w) for lb, v, w in zip(labels, a, b)]
            store_field(0, rows, b, ok)

        def apply(f, base, ok, count=T + 1):
            rows, up, down = row_slices(base)
            c, a = stencil(lambda j, r: V[f, j, r, :], rows, up, down, count)
            if f < 2:
                store_field(f + 1, rows, a, ok)
            return c, a

        def choose(labels, values):
            return jnp.where(labels == 0, values[0], jnp.where(labels == 1, values[1], values[2]))

        def right_side_alone(base):
            rows, up, down = row_slices(base)
            labels = [L[j, rows, :] for j in range(T)]
            b = None
            for k in range(3):
                c = [E[k, j, rows, :] for j in range(T)]
                fwd = [pltpu.roll(v, 1, axis=1) for v in c]
                bwd = [pltpu.roll(v, 127, axis=1) for v in c]
                XE[k, rows, :] = jnp.where(first_lane, fwd[T - 1], bwd[0])
                a = []
                for j in range(T):
                    left = jnp.where(first_lane, fwd[j - 1] if j else 0.0, fwd[j])
                    right = jnp.where(last_lane, bwd[j + 1] if j < T - 1 else 0.0, bwd[j])
                    near = (E[k, j, down, :] + E[k, j, up, :]) + (right + left)
                    a.append(4.0 * c[j] - near)
                b = a if k == 0 else [jnp.where(lb == k, v, w) for lb, v, w in zip(labels, a, b)]
            for j in range(T):
                V[0, j, rows, :] = b[j]

        def right_side_beside(base):
            rows, up, down = row_slices(base)
            fwd = [pltpu.roll(E[k, T, rows, :], 1, axis=1) for k in range(3)]
            bwd = [pltpu.roll(E[k, T, rows, :], 127, axis=1) for k in range(3)]
            a = []
            for k in range(3):
                left = jnp.where(first_lane, XE[k, rows, :], fwd[k])
                right = jnp.where(last_lane, XE[k, rows, :], bwd[k])
                near = (E[k, T, down, :] + E[k, T, up, :]) + (right + left)
                a.append(4.0 * E[k, T, rows, :] - near)
            V[0, T, rows, :] = jnp.where(col_ok, choose(L[T, rows, :], a), 0.0)
            V[0, 0, rows, :] = V[0, 0, rows, :] - jnp.where(first_lane, choose(L[0, rows, :], fwd), 0.0)
            V[0, T - 1, rows, :] = V[0, T - 1, rows, :] - jnp.where(
                last_lane, choose(L[T - 1, rows, :], bwd), 0.0)

        def body(i, carry):
            right_side_alone(pl.multiple_of(8 * i, 8))
            return carry
        lax.fori_loop(1, 17, body, 0, unroll=UNROLL_B)

        def add_up(products):
            while len(products) > 1:
                odd = products[-1:] if len(products) % 2 else []
                products = [a + b for a, b in zip(products[::2], products[1::2])] + odd
            return products[0]

        zero8 = jnp.zeros((8, 128), F32)

        def alone(f, base, inner):
            rows, up, down = row_slices(base)
            c = [V[f, j, rows, :] for j in range(T)]
            fwd = [pltpu.roll(v, 1, axis=1) for v in c]
            bwd = [pltpu.roll(v, 127, axis=1) for v in c]
            a = []
            for j in range(T):
                left = jnp.where(first_lane, fwd[j - 1] if j else 0.0, fwd[j])
                right = jnp.where(last_lane, bwd[j + 1] if j < T - 1 else 0.0, bwd[j])
                near = (V[f, j, down, :] + V[f, j, up, :]) + (right + left)
                a.append(4.0 * c[j] - near)
                if f < 2:
                    V[f + 1, j, rows, :] = a[j]
            if inner:
                return (add_up([c[j] * c[j] for j in range(1, T - 1)]),
                        add_up([c[j] * a[j] for j in range(1, T - 1)]))

        sums = []
        for f in range(3):
            V[f, 0:T, 0:8, :] = jnp.zeros((T, 8, 128), F32)
            V[f, 0:T, 136:144, :] = jnp.zeros((T, 8, 128), F32)
            if f < 2:
                alone(f, 8, False)
                alone(f, 128, False)

            def body(i, carry, f=f):
                got = alone(f, pl.multiple_of(8 * i, 8), True)
                return carry[0] + got[0], carry[1] + got[1]
            sums += list(lax.fori_loop(2, 16, body, (zero8, zero8), unroll=14))
            if f == 0:
                pl.semaphore_wait(known.at[0], len(beside_us))
                two_away = [at(dx=2), at(dy=2), at(dcol=2), at(dcol=-2)]
                for device in two_away:
                    signal(known.at[1], device)

        strips, halo = halo[:2], halo[2:]
        for cp, goes, comes in strips:
            @pl.when(comes)
            def _(cp=cp):
                cp.wait_recv()

        sub32 = lax.broadcasted_iota(jnp.int32, (32, 128), 0) % 8
        merged = jnp.where((sub32 < 4) & has_left, strip_in[0],
                           jnp.where((sub32 >= 4) & has_right, strip_in[1], 0.0))
        beside = jnp.concatenate([merged, jnp.zeros((96, 128), F32)], axis=0).T
        outer = (lane < 4) | (lane >= 124)
        for k in range(4):
            tile = jnp.where(outer, pltpu.roll(beside, 128 - (8 * k + 4), axis=1), 0.0)
            if k < 3:
                E[k, T, 8:136, :] = tile
            else:
                L[T, 8:136, :] = tile.astype(jnp.int32)

        def body(i, carry):
            right_side_beside(pl.multiple_of(8 * i, 8))
            return carry
        lax.fori_loop(1, 17, body, 0, unroll=UNROLL_C)

        for cp, goes, comes in halo:
            @pl.when(comes)
            def _(cp=cp):
                cp.wait_recv()

        for rows, from_left, from_right in ((slice(0, 8), 3, 2), (slice(136, 144), 1, 0)):
            l_ok, r_ok = opposite[from_left], opposite[from_right]
            for k in range(3):
                E[k, T, rows, :] = jnp.where(
                    high4 & l_ok, corner_in[from_left, k],
                    jnp.where(low4 & r_ok, corner_in[from_right, k], 0.0))
            L[T, rows, :] = jnp.where(
                high4 & l_ok, corner_lab[from_left],
                jnp.where(low4 & r_ok, corner_lab[from_right], 0))

        @pl.when(has_up)
        def _():
            for j in range(T):
                for k in range(3):
                    E[k, j, 4:8, :] = RU[k, j, 4:8, :]
                L[j, 4:8, :] = LU[j, 4:8, :]

        @pl.when(has_down)
        def _():
            for j in range(T):
                for k in range(3):
                    E[k, j, 136:140, :] = RD[k, j, 0:4, :]
                L[j, 136:140, :] = LD[j, 0:4, :]

        top_ok = has_up | (sub8 == 7)
        bottom_ok = has_down | (sub8 == 0)
        right_side(1, top_ok)
        right_side(135, bottom_ok)

        def rim(f, base):
            rows, up, down = row_slices(base)
            c = {j: V[f, j, rows, :] for j in (T - 2, T - 1, T, 0, 1)}
            fwd = {j: pltpu.roll(c[j], 1, axis=1) for j in (T - 2, T - 1, T, 0)}
            bwd = {j: pltpu.roll(c[j], 127, axis=1) for j in (T - 1, T, 0, 1)}
            a = {}
            for before, j, after in ((T - 2, T - 1, T), (T - 1, T, 0), (T, 0, 1)):
                if j == T and f == 2:
                    continue
                left = jnp.where(first_lane, fwd[before], fwd[j])
                right = jnp.where(last_lane, bwd[after], bwd[j])
                near = (V[f, j, down, :] + V[f, j, up, :]) + (right + left)
                a[j] = 4.0 * c[j] - near
                if f < 2:
                    V[f + 1, j, rows, :] = jnp.where(col_ok, a[j], 0.0) if j == T else a[j]
            return c[0] * c[0] + c[T - 1] * c[T - 1], c[0] * a[0] + c[T - 1] * a[T - 1]

        for f in range(3):
            if f < 2:
                apply(f, 1, top_ok)
                apply(f, 135, bottom_ok)
            same, next_ = sums[2 * f], sums[2 * f + 1]
            for base in (8, 128):
                c, a = apply(f, base, None, T + 1 if f < 2 else T)
                same = same + add_up([c[j] * c[j] for j in range(T)])
                next_ = next_ + add_up([c[j] * a[j] for j in range(T)])

            def body(i, carry, f=f):
                got = rim(f, pl.multiple_of(8 * i, 8))
                return carry[0] + got[0], carry[1] + got[1]
            sums[2 * f:2 * f + 2] = lax.fori_loop(2, 16, body, (same, next_), unroll=14)

        pairs = [(s, zero8) for s in sums]
        for shift in (4, 2, 1):
            pairs = [pair_add(p, (pltpu.roll(p[0], shift, axis=0), pltpu.roll(p[1], shift, axis=0)))
                     for p in pairs]
        hi, lo = zero8, zero8
        for m, p in enumerate(pairs):
            hi, lo = jnp.where(sub8 == m, p[0], hi), jnp.where(sub8 == m, p[1], lo)
        top = hi.astype(jnp.bfloat16).astype(F32)
        mid = (hi - top).astype(jnp.bfloat16).astype(F32)
        low = (hi - top) - mid
        lo_top = lo.astype(jnp.bfloat16).astype(F32)
        pieces = jnp.concatenate([top, mid, low, lo_top, lo - lo_top], axis=0)
        added = jnp.dot(pieces.astype(jnp.bfloat16), jnp.ones((128, 128), jnp.bfloat16),
                        preferred_element_type=F32).reshape(5, 8, 128)
        hi, lo = two_sum(added[0], added[1])
        hi, lo = two_sum(hi, lo + (added[2] + (added[3] + added[4])))
        line = jnp.where(lane8 == sub8, hi, 0.0) + jnp.where(lane8 == sub8 + 8, lo, 0.0)
        line = jnp.sum(line, axis=0, keepdims=True)

        lane1 = lax.broadcasted_iota(jnp.int32, (1, 128), 1)

        def total(lines):
            err = []
            while len(lines) > 1:
                both = [two_sum(a, b) for a, b in zip(lines[::2], lines[1::2])]
                lines = [b[0] for b in both]
                err += [b[1] for b in both]
            err = add_up(err + [jnp.zeros((1, 128), F32)])
            low = pltpu.roll(lines[0], 120, axis=1) + err
            h, l = two_sum(lines[0], low)
            return jnp.where(lane1 < 8, h, 0.0) + jnp.where(
                (lane1 >= 8) & (lane1 < 16), pltpu.roll(l, 8, axis=1), 0.0)

        def reduce_start(line, buf, phase, me, peers):
            msg[phase] = line
            buf[me] = line

            for device in peers:
                pltpu.make_async_remote_copy(
                    src_ref=msg.at[phase], dst_ref=buf.at[me], send_sem=red_send.at[phase],
                    recv_sem=red_recv.at[phase], device_id=device,
                    device_id_type=MESH).start()

        def reduce_end(buf, phase, n):
            rest = buf.at[pl.ds(0, n - 1)]
            pltpu.make_async_copy(rest, rest, red_recv.at[phase]).wait()
            return total([buf[i] for i in range(n)])

        def reduce_sent(buf, phase, n):
            rest = buf.at[pl.ds(0, n - 1)]
            pltpu.make_async_copy(rest, rest, red_send.at[phase]).wait()

        pl.semaphore_wait(known.at[1], len(two_away))
        signal(known.at[2], at(dcore=1))
        reduce_start(line, red_col, 0, col, [
            at(dcol=d) for d in sorted(range(1, n_col), key=lambda d: -min(d, n_col - d))])

        w4 = weights(512, 4, 1 / 16)
        for h in range(2):
            quads = jnp.concatenate([
                jnp.concatenate([
                    (V[k, 4 * h + j, pl.ds(8, 32, stride=4), :] + V[k, 4 * h + j, pl.ds(9, 32, stride=4), :])
                    + (V[k, 4 * h + j, pl.ds(10, 32, stride=4), :] + V[k, 4 * h + j, pl.ds(11, 32, stride=4), :])
                    for j in range(4)], axis=1) for k in range(3)], axis=0)
            MB[h] = exact_dot(quads, w4).reshape(3, 32, 128)

        def early(h, slot, peer, sem):
            return pltpu.make_async_remote_copy(
                src_ref=MB.at[h], dst_ref=PB.at[slot], send_sem=p_send.at[sem],
                recv_sem=p_recv.at[slot], **to(peer, col))

        pl.semaphore_wait(known.at[2], 1)
        early(1 - core, 2 * jnp.where(core == 0, y, x) + core, row + 1 - 2 * core, 0).start()
        for i in range(1, X):
            early(0, 2 * x + core, (y * X + (x + i) % X) * 2, i).start()
        for i in range(1, n_y):
            early(1, 2 * y + core, (((y + i) % n_y) * X + x) * 2 + 1, X - 1 + i).start()
        own_slot = 2 * jnp.where(core == 0, x, y) + core
        PB[own_slot] = MB[core]

        w2 = weights(256, 2, 0.25)
        def fine_part(j):
            pairs2 = jnp.concatenate([
                jnp.concatenate([V[k, 2 * j + h, pl.ds(8, 64, stride=2), :]
                                 + V[k, 2 * j + h, pl.ds(9, 64, stride=2), :] for h in range(2)], axis=1)
                for k in range(3)], axis=0)
            FB[j] = exact_dot(pairs2, w2).reshape(3, 64, 128)

        fine_part(0)
        fine_part(1)
        line = reduce_end(red_col, 0, n_col)
        reduce_start(line, red_row, 1, row, [
            at(dx=dx, dy=dy, dcore=c) for dx, dy, c in sorted(
                [(dx, dy, c) for dx in range(X) for dy in range(n_y) for c in range(2)][1:],
                key=lambda d: -min(d[0], X - d[0]) - min(d[1], n_y - d[1]) - d[2] / 2)])
        fine_part(2)
        fine_part(3)
        CO[...] = jnp.zeros((n_y, X, 2, 16, 128), F32)
        reduce_sent(red_col, 0, n_col)

        def early_here(i):
            slot = lax.rem(own_slot + i, 8)
            early(0, slot, row, 0).wait_recv()

        for i in range(1, 8):
            early_here(i)
        line = reduce_end(red_row, 1, n_row)

        pick = lambda m: jnp.sum(jnp.where(lane1 == m, line, 0.0), axis=1, keepdims=True)
        n = [(pick(m), pick(m + 8)) for m in range(6)]
        c0, c1, c2 = (jnp.broadcast_to(c, (8, 128)) for c in krylov_weights(n))

        mine = jnp.where(core == 0, y, x)
        for slot in range(8):
            for r in range(4):
                rows = pl.ds(8 * r, 8)
                H[core, mine, slot // 2, slot % 2, rows, :] = (
                    c0 * PB[slot, 0, rows, :] + c1 * PB[slot, 1, rows, :] + c2 * PB[slot, 2, rows, :])

        def late(h, q, peer, sem):
            return pltpu.make_async_remote_copy(
                src_ref=H.at[h, q], dst_ref=H.at[h, q], send_sem=h_send.at[sem],
                recv_sem=h_recv.at[h, q], **to(peer, col))

        partner = row + 1 - 2 * core
        for i in (2, 1, 3):
            peer = jnp.where(core == 0, (((y + i) % n_y) * X + x) * 2, (y * X + (x + i) % X) * 2 + 1)
            late(core, mine, peer, i).start()
        late(core, mine, partner, 0).start()

        def body(i, carry):
            r = pl.multiple_of(8 * i, 8)
            for j in range(T):
                O[j, pl.ds(r, 8), :] = (
                    c0 * V[0, j, pl.ds(r + 8, 8), :] + c1 * V[1, j, pl.ds(r + 8, 8), :]
                    + c2 * V[2, j, pl.ds(r + 8, 8), :])
            return carry
        lax.fori_loop(0, 16, body, 0, unroll=2)

        def body(i, carry):
            rows = pl.ds(pl.multiple_of(8 * i, 8), 8)
            for j in range(T // 2):
                FI[j, rows, :] = (
                    c0 * FB[j, 0, rows, :] + c1 * FB[j, 1, rows, :] + c2 * FB[j, 2, rows, :])
            return carry
        lax.fori_loop(0, 8, body, 0, unroll=2)

        def coarse(h, q):
            rows = [H[h, q, s // 2, s % 2, pl.ds(0, 16, stride=2), :]
                    + H[h, q, s // 2, s % 2, pl.ds(1, 16, stride=2), :] for s in range(8)]
            out = exact_dot(jnp.concatenate(rows, axis=0), weights(128, 2, 0.25, 64 * h))
            for s in range(8):
                at = (jnp.where(h == 0, q, s // 2), jnp.where(h == 0, s // 2, q), s % 2)
                CO[at] = CO[at] + out[16 * s:16 * s + 16, :]

        coarse(core, mine)
        for i in range(7):
            early(0, 0, row, i).wait_send()
        reduce_sent(red_row, 1, n_row)
        for cp, goes, comes in halo + strips:
            @pl.when(goes)
            def _(cp=cp):
                cp.wait_send()

        for i in (1, 3, 2):
            q = (mine + i) % X
            late(core, q, partner, 0).wait_recv()
            late(core, q, partner, X - 1 + i).start()
        for i in (1, 3, 2):
            coarse(core, (mine + i) % X)
        for i in (0, 1, 3, 2):
            q = (jnp.where(core == 0, x, y) + i) % X
            late(1 - core, q, partner, 0).wait_recv()
            coarse(1 - core, q)

        for i in range(7):
            late(0, 0, row, i).wait_send()

    return kernel


def write_out(O, FI, H, CO, o_blend, o_fine, o_mid, o_coarse, sem):
    copies = [(H.at[0, q], o_mid.at[q, :, :, :, pl.ds(0, 128)]) for q in range(X)]
    copies += [(H.at[1, q], o_mid.at[:, q, :, :, pl.ds(128, 128)]) for q in range(X)]
    copies += [(O.at[j], o_blend.at[:, pl.ds(128 * j, 128)]) for j in range(T)]
    copies += [(CO.at[q], o_coarse.at[q]) for q in range(CO.shape[0])]
    copies += [(FI.at[j], o_fine.at[:, pl.ds(128 * j, 128)]) for j in range(T // 2)]
    copies = [pltpu.make_async_copy(a, b, sem.at[i]) for i, (a, b) in enumerate(copies)]
    for cp in copies:
        cp.start()
    for cp in copies:
        cp.wait()


def solution(mesh):
    n_row, n_col = mesh.shape["row"], mesh.shape["col"]

    n_y = n_row // (2 * X)

    def step(sources, labels):
        hbm = pl.BlockSpec(memory_space=pltpu.HBM)
        vmem = pl.BlockSpec(memory_space=pltpu.VMEM)
        sem = pltpu.SemaphoreType.DMA
        parts = pl.pallas_call(
            make_kernel(n_row, n_col),
            out_shape=(
                jax.ShapeDtypeStruct((T, 128, 128), F32),
                jax.ShapeDtypeStruct((T // 2, 64, 128), F32),
                jax.ShapeDtypeStruct((2, 4, 4, 2, 32, 128), F32),
                jax.ShapeDtypeStruct((n_y, X, 2, 16, 128), F32),
            ),
            in_specs=[hbm, hbm],
            out_specs=(vmem, vmem, vmem, vmem),
            scratch_shapes=[
                pltpu.VMEM((3, T + 1, ROWS, 128), F32),
                pltpu.VMEM((T + 1, ROWS, 128), jnp.int32),
                pltpu.VMEM((3, T + 1, ROWS, 128), F32),
                pltpu.VMEM((3, ROWS, 128), F32),
                pltpu.VMEM((3, T, 8, 128), F32),
                pltpu.VMEM((3, T, 8, 128), F32),
                pltpu.VMEM((T, 8, 128), jnp.int32),
                pltpu.VMEM((T, 8, 128), jnp.int32),
                pltpu.VMEM((2, 3, 32, 128), F32),
                pltpu.VMEM((8, 3, 32, 128), F32),
                pltpu.VMEM((T // 2, 3, 64, 128), F32),
                pltpu.VMEM((32, 128), F32),
                pltpu.VMEM((2, 32, 128), F32),
                pltpu.VMEM((4, 3, 8, 128), F32),
                pltpu.VMEM((4, 8, 128), jnp.int32),
                pltpu.VMEM((2, 1, 128), F32),
                pltpu.VMEM((n_row, 1, 128), F32),
                pltpu.VMEM((n_col, 1, 128), F32),
                sem((2 * T,)),
                sem((14,)),
                sem((14,)),
                sem((2,)),
                sem((2,)),
                sem((7,)),
                sem((8,)),
                sem((7,)),
                sem((2, 4)),
                pltpu.SemaphoreType.REGULAR((3,)),
            ],
            compiler_params=pltpu.CompilerParams(
                collective_id=0, has_side_effects=True, vmem_limit_bytes=40 * 1024 * 1024),
        )(pltpu.with_memory_space_constraint(sources, pltpu.HBM), pltpu.with_memory_space_constraint(labels, pltpu.HBM))
        blended, fine, mid, coarse = pl.pallas_call(
            write_out,
            out_shape=(
                jax.ShapeDtypeStruct((128, 1024), F32),
                jax.ShapeDtypeStruct((64, 512), F32),
                jax.ShapeDtypeStruct((n_y, X, 2, 32, 256), F32),
                jax.ShapeDtypeStruct((n_y, X, 2, 16, 128), F32),
            ),
            in_specs=[vmem] * 4,
            out_specs=(hbm,) * 4,
            scratch_shapes=[sem((2 * X + T + n_y + T // 2,))],
            compiler_params=pltpu.CompilerParams(vmem_limit_bytes=1024 * 1024),
        )(*parts)
        return blended, fine, mid.reshape(-1, 256), coarse.reshape(-1, 128)

    return jax.shard_map(
        step,
        mesh=mesh,
        in_specs=(P(None, "row", "col"), P("row", "col")),
        out_specs=(P("row", "col"), P("row", "col"), P(None, "col"), P(None, "col")),
        check_vma=False,
    )
```
